128 devices in a mesh: dp: 16 (over x, z), expert: 8 (over y, core).
Axes of the slice: x: 4, y: 4, z: 4, core: 2. Of those that a mesh axis runs over, the one named last changes fastest.
Arguments:
- tokens: bfloat16 [16384, 2048], P(('dp', 'expert')), may hold values from -6 to 6
- out_grad: bfloat16 [16384, 2048], P(('dp', 'expert')), may hold values from -3 to 3
- z_weight: float32 [16384], P(('dp', 'expert')), may hold values from 0.1 to 1
- router_weight: bfloat16 [2048, 128], replicated, may hold values from -0.125 to 0.125
- expert_ids: int32 [16384, 4], P(('dp', 'expert')), may hold values from 0 to 127, as said below
- gate_up_weight: bfloat16 [8, 2048, 3072], P('expert'), may hold values from -0.125 to 0.125
- down_weight: bfloat16 [8, 1536, 2048], P('expert'), may hold values from -0.15625 to 0.15625
Outputs:
- token_grad: bfloat16 [16384, 2048], P(('dp', 'expert'))
- router_grad: float32 [2048, 128], replicated
- gate_up_grad: bfloat16 [8, 2048, 3072], P('expert', 'dp')
- down_grad: bfloat16 [8, 1536, 2048], P('expert', 'dp')
The draws below stay inside these ranges and needn't reach their ends.
Inputs may be any that keep to these rules, and one draw needn't show every extreme that they name: `expert_ids`: each row names 4 different experts. Experts 0 to 7 are the ones in flight. The 128 rows of one device name any one expert in flight at most 64 times; in every data group some expert in flight is named exactly 64 times by the rows of each device of the group.
All inputs are finite; a program needn't handle non-finite values.
Results may differ from the reference program's by a relative error of at most 0.019.
Values may be sent and summed in bfloat16 or wider, within the bound.
A program may use at most 192 MiB of HBM per device.

```python
import math
import jax
import jax.numpy as jnp
from jax import lax

D = 2048
FF = 1536
ROUTED = 128
TOP = 4
BLOCK = 128
TOK_DEV = 128
CAP = 64
FLIGHT = 8
TOKENS = 16384
N_DP = 16
N_EXPERT = 8


def draw_expert_ids(key, part):
    devices_all = TOKENS // TOK_DEV
    flight = N_EXPERT
    key_base, key_mask, key_hot, key_dev = jax.random.split(key, 4)
    base = jax.random.randint(key_base, (devices_all, flight), 0, CAP + 1)
    base = base * jax.random.randint(key_mask, (devices_all, flight), 0, 2)
    hot = jax.random.randint(key_hot, (devices_all // N_EXPERT,), 0, flight)
    hot_dev = jnp.repeat(hot, N_EXPERT)
    counts = jnp.where(jnp.arange(flight)[None, :] == hot_dev[:, None], CAP, base).astype(jnp.int32)
    others = ROUTED - flight
    spacing = others // TOP

    def one_device(count_row, dev_key):
        key_fill, key_order, key_perm = jax.random.split(dev_key, 3)
        ends = jnp.cumsum(count_row)
        total = ends[-1]
        demand = jnp.arange(TOP * TOK_DEV, dtype=jnp.int32)
        owner = jnp.sum((ends[None, :] <= demand[:, None]).astype(jnp.int32), axis=1)
        table = jnp.where(demand < total, owner, -1).reshape(TOP, TOK_DEV).T
        offset = jax.random.randint(key_fill, (TOK_DEV, 1), 0, others)
        fill = flight + (offset + jnp.arange(TOP, dtype=jnp.int32)[None, :] * spacing) % others
        table = jnp.where(table >= 0, table, fill)
        order_keys = jax.random.randint(key_order, (TOK_DEV, TOP), 0, 1 << 20) * TOP + jnp.arange(TOP, dtype=jnp.int32)[None, :]
        order = jnp.argsort(order_keys, axis=1, stable=True)
        table = jnp.take_along_axis(table, order, axis=1)
        shuffle = jax.random.permutation(key_perm, TOK_DEV)
        return table[shuffle]
    dev_keys = jax.random.split(key_dev, devices_all)
    result = jax.vmap(one_device)(counts, dev_keys)
    return result.reshape(TOKENS, TOP).astype(jnp.int32)


def block_levels(rng, dims, cuts, smallest, high):
    level = 1.0
    for position, shards_of in cuts:
        heights = jax.random.uniform(jax.random.fold_in(jax.random.fold_in(rng, 6), position), (shards_of,), jnp.float32, smallest / len(cuts), high / len(cuts))
        level = level * jnp.repeat(jnp.exp(heights), dims[position] // shards_of).reshape((-1,) + (1,) * (len(dims) - 1 - position))
    return level


def normal_values(rng, extent, scale, limit, shards=(), kind=jnp.bfloat16):
    entries = scale * jax.random.normal(rng, extent, jnp.float32)
    if shards:
        entries = entries * block_levels(rng, extent, shards, -0.22, 0.18)
    return jnp.clip(entries, -limit, limit).astype(kind)


def setup_inputs(seed: int = 0) -> dict:
    key_list = jax.random.split(jax.random.key(seed), 8)
    tokens = normal_values(key_list[0], (TOKENS, D), 1.0, 6.0, ((0, 128),))
    out_grad = normal_values(key_list[1], (TOKENS, D), 0.5, 3.0, ((0, 128),))
    z_weight = jnp.clip(jnp.exp(math.log(1.0) - 2.3025851 * jax.random.uniform(key_list[2], (TOKENS,), jnp.float32) ** block_levels(key_list[2], (TOKENS,), ((0, 128),), -0.2, 0.2)), 0.1, 1.0)
    router_weight = normal_values(key_list[3], (D, ROUTED), D ** -0.5, 0.125)
    expert_ids = draw_expert_ids(jax.random.fold_in(key_list[7], 71), 0)
    gate_up_weight = normal_values(key_list[5], (FLIGHT, D, 2 * FF), D ** -0.5, 0.125, ((0, 8),))
    down_weight = normal_values(key_list[6], (FLIGHT, FF, D), FF ** -0.5, 0.15625, ((0, 8),))
    return dict(tokens=tokens, out_grad=out_grad, z_weight=z_weight, router_weight=router_weight, expert_ids=expert_ids, gate_up_weight=gate_up_weight, down_weight=down_weight)


def expert_rows(rows_in, rows_grad, w_gateup, w_down, acc_gateup, acc_down):
    hidden_units = w_down.shape[0]
    pre_act = jnp.dot(rows_in, w_gateup, preferred_element_type=jnp.float32)
    gate_pre = pre_act[:, :hidden_units]
    up_pre = pre_act[:, hidden_units:]
    activated = jax.nn.silu(gate_pre)
    hidden = (activated * up_pre).astype(jnp.bfloat16)
    expert_out = jnp.dot(hidden, w_down, preferred_element_type=jnp.float32).astype(jnp.bfloat16)
    hidden_grad = lax.dot_general(rows_grad, w_down, (((1,), (1,)), ((), ())), preferred_element_type=jnp.float32)
    acc_down = acc_down + lax.dot_general(hidden, rows_grad, (((0,), (0,)), ((), ())), preferred_element_type=jnp.float32)
    sigmoid_gate = jax.nn.sigmoid(gate_pre)
    gate_grad = hidden_grad * up_pre * sigmoid_gate * (1.0 + gate_pre * (1.0 - sigmoid_gate))
    up_grad = hidden_grad * activated
    pre_grad = jnp.concatenate([gate_grad, up_grad], axis=1).astype(jnp.bfloat16)
    acc_gateup = acc_gateup + lax.dot_general(rows_in, pre_grad, (((0,), (0,)), ((), ())), preferred_element_type=jnp.float32)
    input_grad = lax.dot_general(pre_grad, w_gateup, (((1,), (1,)), ((), ())), preferred_element_type=jnp.float32).astype(jnp.bfloat16)
    return acc_gateup, acc_down, expert_out, input_grad


def run_blocks(work_in, work_grad, w_gateup, w_down, nblocks):
    width = work_in.shape[1]
    hidden_units = w_down.shape[0]
    start_state = (jnp.zeros((width, 2 * hidden_units), jnp.float32), jnp.zeros((hidden_units, width), jnp.float32),
                   jnp.zeros_like(work_in), jnp.zeros_like(work_in))

    def step(block_index, carry):
        acc_gateup, acc_down, out_rows, grad_rows = carry
        start = (block_index * BLOCK).astype(jnp.int32)
        rows_in = lax.dynamic_slice_in_dim(work_in, start, BLOCK, 0)
        rows_grad = lax.dynamic_slice_in_dim(work_grad, start, BLOCK, 0)
        acc_gateup, acc_down, produced, backward = expert_rows(rows_in, rows_grad, w_gateup, w_down, acc_gateup, acc_down)
        out_rows = lax.dynamic_update_slice_in_dim(out_rows, produced, start, 0)
        grad_rows = lax.dynamic_update_slice_in_dim(grad_rows, backward, start, 0)
        return acc_gateup, acc_down, out_rows, grad_rows

    return lax.fori_loop(jnp.int32(0), nblocks.astype(jnp.int32), step, start_state)


def reference(tokens, out_grad, z_weight, router_weight, expert_ids, gate_up_weight, down_weight):
    logits = jnp.dot(tokens, router_weight, preferred_element_type=jnp.float32)
    choose = expert_ids[:, :, None] == jnp.arange(ROUTED, dtype=jnp.int32)[None, None, :]
    selected = jnp.sum(jnp.where(choose, logits[:, None, :], 0.0), axis=2)
    sel_exp = jnp.exp(selected)
    probs = sel_exp / jnp.sum(sel_exp, axis=1, keepdims=True)
    log_total = jnp.log(jnp.sum(jnp.exp(logits), axis=1))
    slots_group = N_EXPERT * TOK_DEV * TOP
    rows_max = N_EXPERT * CAP
    group_ids = expert_ids.reshape(N_DP, slots_group)
    group_prob = probs.reshape(N_DP, slots_group)
    group_tok = tokens.reshape(N_DP, N_EXPERT * TOK_DEV, D)
    group_grad = out_grad.reshape(N_DP, N_EXPERT * TOK_DEV, D)

    def one_group(carry, data):
        ids_here, prob_here, tok_here, grad_here = data

        def one_expert(expert):
            member = ids_here == expert
            rank = jnp.cumsum(member.astype(jnp.int32)) - 1
            place = jnp.where(member, rank, rows_max).astype(jnp.int32)
            source = jnp.zeros((rows_max,), jnp.int32).at[place].set(jnp.arange(slots_group, dtype=jnp.int32), mode="drop")
            valid = jnp.zeros((rows_max,), jnp.bool_).at[place].set(True, mode="drop")
            tok_index = source // TOP
            rows_in = jnp.where(valid[:, None], tok_here[tok_index], 0)
            rows_grad = jnp.where(valid[:, None], prob_here[source][:, None] * grad_here[tok_index].astype(jnp.float32), 0.0).astype(jnp.bfloat16)
            used = (jnp.sum(member.astype(jnp.int32)) + BLOCK - 1) // BLOCK
            acc_gateup, acc_down, produced, backward = run_blocks(rows_in, rows_grad, gate_up_weight[expert], down_weight[expert], used)
            return acc_gateup.astype(jnp.bfloat16), acc_down.astype(jnp.bfloat16), produced, backward, source, valid

        part_gu, part_down, outs, backs, sources, valids = lax.map(one_expert, jnp.arange(N_EXPERT, dtype=jnp.int32))
        sum_gu, sum_down = carry
        sum_gu = sum_gu + part_gu.astype(jnp.float32)
        sum_down = sum_down + part_down.astype(jnp.float32)
        target = jnp.where(valids.reshape(-1), sources.reshape(-1), slots_group).astype(jnp.int32)
        slot_out = jnp.zeros((slots_group, D), jnp.bfloat16).at[target].set(outs.reshape(-1, D), mode="drop")
        slot_back = jnp.zeros((slots_group, D), jnp.bfloat16).at[target].set(backs.reshape(-1, D), mode="drop")
        return (sum_gu, sum_down), (slot_out, slot_back)

    start_sums = (jnp.zeros((N_EXPERT, D, 2 * FF), jnp.float32), jnp.zeros((N_EXPERT, FF, D), jnp.float32))
    (sum_gu, sum_down), (slot_out, slot_back) = lax.scan(one_group, start_sums, (group_ids, group_prob, group_tok, group_grad))
    slot_out = slot_out.reshape(TOKENS, TOP, D)
    slot_back = slot_back.reshape(TOKENS, TOP, D)
    scores = jnp.sum(out_grad[:, None, :].astype(jnp.float32) * slot_out.astype(jnp.float32), axis=2)
    mean_score = jnp.sum(probs * scores, axis=1, keepdims=True)
    sel_grad = probs * (scores - mean_score)
    z_grad = 2.0 * z_weight[:, None] * log_total[:, None] * jnp.exp(logits - log_total[:, None])
    logit_grad = (z_grad + jnp.sum(jnp.where(choose, sel_grad[:, :, None], 0.0), axis=1)).astype(jnp.bfloat16)
    token_grad = (jnp.sum(slot_back.astype(jnp.float32), axis=1)
                  + lax.dot_general(logit_grad, router_weight, (((1,), (1,)), ((), ())), preferred_element_type=jnp.float32)).astype(jnp.bfloat16)
    router_grad = lax.dot_general(tokens, logit_grad, (((0,), (0,)), ((), ())), preferred_element_type=jnp.float32)
    return token_grad, router_grad, sum_gu.astype(jnp.bfloat16), sum_down.astype(jnp.bfloat16)
```

```python
import functools

import jax
import jax.numpy as jnp
from jax import lax
from jax.experimental import pallas as pl
from jax.experimental.pallas import tpu as pltpu
from jax.sharding import PartitionSpec as P

BF = jnp.bfloat16
F32 = jnp.float32
MESH = pl.DeviceIdType.MESH

TOK = 128
CAP = 64
D = 2048
FF = 1536
SRC = 8
ROWS = SRC * CAP
ROUTED = 128
ND = D // 256
NG = 2 * FF // 256
NC = ND + NG
LAG1, LAG2, LAG3, LAG4 = 1, 3, 4, 6
DEP = 6
RING = 8
INV = (0, 1, 4, 5, 2, 3, 6, 7)


def nt(a, b):
    return lax.dot_general(a, b, (((1,), (1,)), ((), ())), preferred_element_type=F32)


def tn(a, b):
    return lax.dot_general(a, b, (((0,), (0,)), ((), ())), preferred_element_type=F32)


def nn(a, b):
    return jnp.dot(a, b, preferred_element_type=F32)


def kernel(
    tokens_hbm, grad_hbm, z_ref, rw_ref, ids_ref, gu_hbm, dn_hbm,
    tg_out, lg_out, gug_out, dng_out,
    xa, oa, meta, prob, logit, xr, xt, dy, hid, hidt, pg, gu, dn,
    part, r1, r2, rg, rb, sel, psum, psend, precv,
    lsem, ag_s, ag_r, mt_s, mt_r, ps_s, ps_r, rt_s, rt_r, s1, q1, s2, q2,
):
    dp = lax.axis_index("dp")
    ex = lax.axis_index("expert")
    px, pz = dp // 4, dp % 4
    py, pc = ex // 2, ex % 2
    xp, xm = ((px + 1) % 4) * 4 + pz, ((px + 3) % 4) * 4 + pz
    zp, zm = px * 4 + (pz + 1) % 4, px * 4 + (pz + 3) % 4
    yp, ym, yo = (py + 1) % 4, (py + 3) % 4, (py + 2) % 4
    oc = 1 - pc
    place = (ex, py * 2 + oc, ym * 2 + pc, ym * 2 + oc, yp * 2 + pc, yp * 2 + oc, yo * 2 + pc, yo * 2 + oc)

    cp_tok = pltpu.make_async_copy(tokens_hbm, xa.at[0], lsem.at[0])
    cp_grad = pltpu.make_async_copy(grad_hbm, oa.at[0], lsem.at[1])
    cp_gu = pltpu.make_async_copy(gu_hbm, gu, lsem.at[2])
    cp_dn = pltpu.make_async_copy(dn_hbm, dn, lsem.at[3])
    cp_tok.start()
    cp_grad.start()
    cp_gu.start()
    cp_dn.start()

    barrier = pltpu.get_barrier_semaphore()
    for to in (xp, xm, zp, zm):
        pl.semaphore_signal(barrier, inc=1, device_id=(to, ex), device_id_type=MESH)
    for q in range(1, SRC):
        pl.semaphore_signal(barrier, inc=1, device_id=(dp, place[q]), device_id_type=MESH)
    pl.semaphore_wait(barrier, 4 + SRC - 1)

    def ag(arr, buf, src_q, half, to_q, dst_q, k):
        rows = pl.ds(half * CAP, CAP)
        return pltpu.make_async_remote_copy(
            src_ref=buf.at[src_q, rows], dst_ref=buf.at[dst_q, rows],
            send_sem=ag_s.at[arr, k], recv_sem=ag_r.at[arr, dst_q, half],
            device_id=(dp, place[to_q]), device_id_type=MESH,
        )

    def ag_wait(arr, buf, q, half):
        rows = pl.ds(half * CAP, CAP)
        pltpu.make_async_remote_copy(
            src_ref=buf.at[q, rows], dst_ref=buf.at[q, rows],
            send_sem=ag_s.at[arr, 0], recv_sem=ag_r.at[arr, q, half],
            device_id=(dp, place[1]), device_id_type=MESH,
        ).wait_recv()

    def ag_own(arr, buf):
        out = [
            ag(arr, buf, 0, 0, 4, 2, 0), ag(arr, buf, 0, 1, 2, 4, 1),
            ag(arr, buf, 0, 1, 4, 2, 2), ag(arr, buf, 0, 0, 2, 4, 3),
            ag(arr, buf, 0, 0, 1, 1, 4), ag(arr, buf, 0, 1, 1, 1, 5),
        ]
        for c in out:
            c.start()
        return out

    def ag_relay(arr, buf):
        ag_wait(arr, buf, 2, 0)
        a = ag(arr, buf, 2, 0, 4, 6, 6)
        a.start()
        b = ag(arr, buf, 2, 0, 1, 3, 8)
        b.start()
        ag_wait(arr, buf, 4, 1)
        c = ag(arr, buf, 4, 1, 2, 6, 7)
        c.start()
        d = ag(arr, buf, 4, 1, 1, 5, 9)
        d.start()
        return [a, b, c, d]

    def ag_near(arr, buf):
        ag_wait(arr, buf, 2, 1)
        a = ag(arr, buf, 2, 1, 1, 3, 10)
        a.start()
        ag_wait(arr, buf, 4, 0)
        b = ag(arr, buf, 4, 0, 1, 5, 11)
        b.start()
        return [a, b]

    def ag_far(arr, buf):
        out = []
        for half in range(2):
            ag_wait(arr, buf, 6, half)
            a = ag(arr, buf, 6, half, 1, 7, 12 + half)
            a.start()
            out.append(a)
        return out

    def ag_side(arr, buf, q):
        ag_wait(arr, buf, q, 0)
        ag_wait(arr, buf, q, 1)

    sent = []
    cp_tok.wait()
    sent += ag_own(0, xa)

    sub = lax.broadcasted_iota(jnp.int32, (TOK, TOK), 0)
    lane = lax.broadcasted_iota(jnp.int32, (TOK, TOK), 1)
    lg = nn(xa[0], rw_ref[...])
    logit[...] = lg
    ids = ids_ref[...]
    dense = jnp.zeros((TOK, ROUTED), F32)
    mask = jnp.zeros((TOK, ROUTED), F32)
    total = jnp.zeros((TOK, 1), F32)
    for k in range(4):
        hit = ids[:, k : k + 1] == lane
        value = jnp.exp(jnp.sum(jnp.where(hit, lg, 0.0), axis=1, keepdims=True))
        total = total + value
        dense = jnp.where(hit, value, dense)
        mask = jnp.where(hit, 1.0, mask)
    dense = dense / total
    prob[...] = dense
    before = jnp.where(lane < sub, 1.0, 0.0).astype(BF)
    rank = nn(before, mask.astype(BF))
    rank = jnp.where(mask > 0.5, rank, -1.0)
    meta[0, 0:8, :] = dense.T[0:8]
    meta[0, 8:16, :] = rank.T[0:8]
    meta_sent = []
    for q in range(1, SRC):
        c = pltpu.make_async_remote_copy(
            src_ref=meta.at[0], dst_ref=meta.at[INV[q]], send_sem=mt_s.at[q], recv_sem=mt_r.at[INV[q]],
            device_id=(dp, place[q]), device_id_type=MESH,
        )
        c.start()
        meta_sent.append(c)

    sent += ag_relay(0, xa)
    cp_grad.wait()
    sent += ag_own(1, oa)
    sent += ag_near(0, xa)

    for q in range(1, SRC):
        pltpu.make_async_remote_copy(
            src_ref=meta.at[0], dst_ref=meta.at[q], send_sem=mt_s.at[q], recv_sem=mt_r.at[q],
            device_id=(dp, place[q]), device_id_type=MESH,
        ).wait_recv()

    slot_of = lax.broadcasted_iota(jnp.int32, (CAP, TOK), 0).astype(F32)

    def pick(q):
        return (slot_of == meta[q, pl.ds(8 + ex, 1), :]).astype(F32)

    def gather_tok(q):
        rows = nn(pick(q).astype(BF), xa[q]).astype(BF)
        xr[q * CAP : (q + 1) * CAP, :] = rows

    def gather_grad(q):
        p = pick(q)
        weight = jnp.sum(p * meta[q, pl.ds(ex, 1), :], axis=1, keepdims=True)
        rows = nn(p.astype(BF), oa[q])
        dy[q * CAP : (q + 1) * CAP, :] = (weight * rows).astype(BF)

    for q in (1, 3, 5):
        ag_side(0, xa, q)
    for q in range(6):
        gather_tok(q)
    sent += ag_far(0, xa)
    gather_tok(6)
    ag_side(0, xa, 7)
    gather_tok(7)
    cp_gu.wait()

    def forward(f, _):
        a = pl.ds(pl.multiple_of(f * 256, 256), 256)
        b = pl.ds(pl.multiple_of(FF + f * 256, 256), 256)
        g = nn(xr[...], gu[:, a])
        u = nn(xr[...], gu[:, b])
        s = lax.logistic(g)
        act = g * s
        h = (act * u).astype(BF)
        hid[:, a] = h
        hidt[a, :] = h.T
        pg[:, a] = (u * s * (1.0 + g * (1.0 - s))).astype(BF)
        pg[:, b] = act.astype(BF)
        return 0

    lax.fori_loop(0, 3, forward, 0)
    sent += ag_relay(1, oa)
    lax.fori_loop(3, 6, forward, 0)
    sent += ag_near(1, oa)

    def flip(k, _):
        a = pl.ds(pl.multiple_of(k * 256, 256), 256)
        xt[a, :] = xr[:, a].T
        return 0

    lax.fori_loop(0, D // 256, flip, 0)
    for q in (1, 3, 5):
        ag_side(1, oa, q)
    for q in range(6):
        gather_grad(q)
    sent += ag_far(1, oa)
    gather_grad(6)
    ag_side(1, oa, 7)
    gather_grad(7)
    cp_dn.wait()
    for c in sent:
        c.wait_send()
    for c in meta_sent:
        c.wait_send()

    axes = (((xp, xm, px), (zp, zm, pz)), ((zp, zm, pz), (xp, xm, px)))

    def send1(col, kind, slot, ring, zr):
        plus, minus, fc = axes[col][0]
        base = (
            ((fc + 2) % 4) * 4, ((fc + 2) % 4) * 4 + 2,
            ((fc + 1) % 4) * 4 + 2, ((fc + 3) % 4) * 4,
            ((fc + 1) % 4) * 4, ((fc + 3) % 4) * 4 + 2,
        )[kind]
        return pltpu.make_async_remote_copy(
            src_ref=part.at[ring, col, pl.ds(base, 2), pl.ds(0, zr)],
            dst_ref=r1.at[slot, col, kind, :, pl.ds(0, zr)],
            send_sem=s1.at[slot, col, kind], recv_sem=q1.at[slot, col, kind],
            device_id=(plus if kind % 2 == 0 else minus, ex), device_id_type=MESH,
        )

    def send2(col, kind, slot, ring, zr):
        plus, minus, sc = axes[col][1]
        fc = axes[col][0][2]
        h = zr // 2
        step, low = ((2, 0), (2, h), (1, h), (3, 0), (1, 0), (3, h))[kind]
        return pltpu.make_async_remote_copy(
            src_ref=part.at[ring, col, fc * 4 + (sc + step) % 4, pl.ds(low, h)],
            dst_ref=r2.at[slot, col, kind, pl.ds(0, h)],
            send_sem=s2.at[slot, col, kind], recv_sem=q2.at[slot, col, kind],
            device_id=(plus if kind % 2 == 0 else minus, ex), device_id_type=MESH,
        )

    def f32(v):
        return v.astype(F32)

    def compute(c, lhs, rhs_of, zr):
        slot, ring = c % DEP, c % RING
        rhs = rhs_of(c)
        rows = 4 * zr

        def one(b, _):
            r = nn(lhs[pl.ds(pl.multiple_of(b * rows, rows), rows), :], rhs).astype(BF)
            for k in range(4):
                part[ring, 0, b * 4 + k, 0:zr] = r[k * zr : (k + 1) * zr, 0:128]
                part[ring, 1, k * 4 + b, 0:zr] = r[k * zr : (k + 1) * zr, 128:256]
            return 0

        lax.fori_loop(0, 4, one, 0)
        for kind in range(4):
            for col in range(2):
                send1(col, kind, slot, ring, zr).start()

    def stage1(c, zr):
        slot, ring = c % DEP, c % RING
        for col in range(2):
            fc = axes[col][0][2]
            for kind in range(2):
                send1(col, kind, slot, ring, zr).wait_recv()
                base = ((fc + 1) % 4) * 4 if kind == 0 else ((fc + 3) % 4) * 4 + 2
                at = (ring, col, pl.ds(base, 2), pl.ds(0, zr))
                part[at] = (f32(part[at]) + f32(r1[slot, col, kind, :, 0:zr])).astype(BF)
                send1(col, 4 + kind, slot, ring, zr).start()

    def stage2(c, zr):
        slot, ring = c % DEP, c % RING
        for col in range(2):
            fc = axes[col][0][2]
            for kind in range(2, 6):
                send1(col, kind, slot, ring, zr).wait_recv()
            for half, (a, b) in enumerate(((4, 3), (2, 5))):
                at = (ring, col, pl.ds(fc * 4 + 2 * half, 2), pl.ds(0, zr))
                part[at] = (
                    f32(part[at]) + f32(r1[slot, col, a, :, 0:zr]) + f32(r1[slot, col, b, :, 0:zr])
                ).astype(BF)
            for kind in range(4):
                send1(col, kind, slot, ring, zr).wait_send()
            for kind in range(4):
                send2(col, kind, slot, ring, zr).start()

    def stage3(c, zr):
        slot, ring = c % DEP, c % RING
        h = zr // 2
        for col in range(2):
            fc, sc = axes[col][0][2], axes[col][1][2]
            for kind in range(2):
                send2(col, kind, slot, ring, zr).wait_recv()
                step, low = ((1, 0), (3, h))[kind]
                at = (ring, col, fc * 4 + (sc + step) % 4, pl.ds(low, h))
                part[at] = (f32(part[at]) + f32(r2[slot, col, kind, 0:h])).astype(BF)
                send2(col, 4 + kind, slot, ring, zr).start()
            for kind in range(4, 6):
                send1(col, kind, slot, ring, zr).wait_send()

    def stage4(c, zr, out, first):
        slot, ring = c % DEP, c % RING
        h = zr // 2
        for col in range(2):
            fc, sc = axes[col][0][2], axes[col][1][2]
            for kind in range(2, 6):
                send2(col, kind, slot, ring, zr).wait_recv()
            cols = pl.ds(pl.multiple_of((c - first) * 256 + col * 128, 128), 128)
            for half, (a, b) in enumerate(((4, 3), (2, 5))):
                own = part[ring, col, fc * 4 + sc, half * h : (half + 1) * h]
                out[half * h : (half + 1) * h, cols] = (
                    f32(own) + f32(r2[slot, col, a, 0:h]) + f32(r2[slot, col, b, 0:h])
                ).astype(BF)
            for kind in range(6):
                send2(col, kind, slot, ring, zr).wait_send()

    def both(c, fn, on_down, on_gate):
        @pl.when(jnp.logical_and(c >= 0, c < ND))
        def _():
            fn(c, *on_down)

        @pl.when(jnp.logical_and(c >= ND, c < NC))
        def _():
            fn(c, *on_gate)

    ZD, ZG = FF // 16, D // 16

    def down_rhs(c):
        return dy[:, pl.ds(pl.multiple_of(c * 256, 256), 256)]

    def gate_rhs(c):
        return pg[:, pl.ds(pl.multiple_of((c - ND) * 256, 256), 256)]

    def hidden_grad(f):
        a = pl.ds(pl.multiple_of(f * 256, 256), 256)
        b = pl.ds(pl.multiple_of(FF + f * 256, 256), 256)
        hg = nt(dy[...], dn[a, :])
        score = jnp.sum(f32(hid[:, a]) * hg, axis=1, keepdims=True)
        psum[...] = jnp.where(f == 0, 0.0, psum[...]) + score
        pg[:, a] = (f32(pg[:, a]) * hg).astype(BF)
        pg[:, b] = (f32(pg[:, b]) * hg).astype(BF)

    def ps_copy(q):
        return pltpu.make_async_remote_copy(
            src_ref=psend.at[q], dst_ref=precv.at[INV[q]], send_sem=ps_s.at[q], recv_sem=ps_r.at[INV[q]],
            device_id=(dp, place[q]), device_id_type=MESH,
        )

    def send_scores():
        for q in range(SRC):
            row = jnp.sum(pick(q) * psum[q * CAP : (q + 1) * CAP, :], axis=0, keepdims=True)
            if q == 0:
                precv[0] = jnp.broadcast_to(row, (8, TOK))
            else:
                psend[q] = jnp.broadcast_to(row, (8, TOK))
        for q in range(1, SRC):
            ps_copy(q).start()

    def row_grad(k):
        def one(j, _):
            at = pl.ds(pl.multiple_of((k * 2 + j) * 256, 256), 256)
            rg[:, at] = nt(pg[...], gu[at, :]).astype(BF)
            return 0

        lax.fori_loop(0, 2, one, 0)

    def rt_copy(q):
        return pltpu.make_async_remote_copy(
            src_ref=rg.at[pl.ds(q * CAP, CAP)], dst_ref=rb.at[pl.ds(INV[q] * CAP, CAP)],
            send_sem=rt_s.at[q], recv_sem=rt_r.at[INV[q]],
            device_id=(dp, place[q]), device_id_type=MESH,
        )

    def rt_wait(q):
        pltpu.make_async_remote_copy(
            src_ref=rg.at[pl.ds(q * CAP, CAP)], dst_ref=rb.at[pl.ds(q * CAP, CAP)],
            send_sem=rt_s.at[q], recv_sem=rt_r.at[q],
            device_id=(dp, place[q]), device_id_type=MESH,
        ).wait_recv()

    def send_rows():
        for q in range(1, SRC):
            rt_copy(q).start()
        rb[0:CAP, :] = rg[0:CAP, :]

    def logit_grad():
        for q in range(1, SRC):
            pltpu.make_async_remote_copy(
                src_ref=psend.at[q], dst_ref=precv.at[q], send_sem=ps_s.at[q], recv_sem=ps_r.at[q],
                device_id=(dp, place[q]), device_id_type=MESH,
            ).wait_recv()
        for q in range(1, SRC):
            ps_copy(q).wait_send()
        scores = jnp.zeros((ROUTED, TOK), F32)
        for q in range(SRC):
            scores = jnp.where(sub == place[q], precv[q, 0:1, :], scores)
        scores = scores.T
        mean = jnp.sum(scores, axis=1, keepdims=True)
        z = jnp.sum(jnp.where(sub == lane, z_ref[...], 0.0), axis=1, keepdims=True)
        lgt = logit[...]
        log_total = jnp.log(jnp.sum(jnp.exp(lgt), axis=1, keepdims=True))
        z_grad = 2.0 * z * log_total * jnp.exp(lgt - log_total)
        lg_out[...] = (z_grad + scores - prob[...] * mean).astype(BF)

    def token_grad():
        for q in range(1, SRC):
            rt_wait(q)
        for q in range(1, SRC):
            rt_copy(q).wait_send()
        for q in range(SRC):
            sel[q * CAP : (q + 1) * CAP, :] = (
                slot_of == meta[0, pl.ds(8 + place[q], 1), :]
            ).astype(F32).astype(BF)
        chosen = sel[...]
        grad = lg_out[...]

        def one(k, _):
            at = pl.ds(pl.multiple_of(k * 256, 256), 256)
            tg_out[:, at] = (tn(chosen, rb[:, at]) + nt(grad, rw_ref[at, :])).astype(BF)
            return 0

        lax.fori_loop(0, D // 256, one, 0)

    def body(i, _):
        @pl.when(i < ND)
        def _():
            compute(i, hidt, down_rhs, ZD)

        @pl.when(jnp.logical_and(i >= ND, i < NC))
        def _():
            compute(i, xt, gate_rhs, ZG)

        @pl.when(i < 6)
        def _():
            hidden_grad(i)

        @pl.when(i == 6)
        def _():
            send_scores()

        @pl.when(jnp.logical_and(i >= ND, i < ND + 4))
        def _():
            row_grad(i - ND)

        @pl.when(i == ND + 3)
        def _():
            send_rows()

        @pl.when(i == ND + 4)
        def _():
            logit_grad()

        @pl.when(i == NC)
        def _():
            token_grad()

        c4 = i - LAG4

        @pl.when(jnp.logical_and(c4 >= 0, c4 < ND))
        def _():
            stage4(c4, ZD, dng_out, 0)

        @pl.when(c4 >= ND)
        def _():
            stage4(c4, ZG, gug_out, ND)

        both(i - LAG3, stage3, (ZD,), (ZG,))
        both(i - LAG2, stage2, (ZD,), (ZG,))
        both(i - LAG1, stage1, (ZD,), (ZG,))
        return 0

    lax.fori_loop(0, NC + LAG4, body, 0)


def per_device(tokens, out_grad, z_weight, router_weight, expert_ids, gate_up_weight, down_weight):
    vmem = pl.BlockSpec(memory_space=pltpu.VMEM)
    hbm = pl.BlockSpec(memory_space=pl.ANY)
    dma = pltpu.SemaphoreType.DMA
    token_grad, logit_grad, gate_up_grad, down_grad = pl.pallas_call(
        kernel,
        out_shape=(
            jax.ShapeDtypeStruct((TOK, D), BF),
            jax.ShapeDtypeStruct((TOK, ROUTED), BF),
            jax.ShapeDtypeStruct((D // 16, 2 * FF), BF),
            jax.ShapeDtypeStruct((FF // 16, D), BF),
        ),
        in_specs=[hbm, hbm, vmem, vmem, vmem, hbm, hbm],
        out_specs=(vmem, vmem, vmem, vmem),
        scratch_shapes=[
            pltpu.VMEM((SRC, TOK, D), BF),
            pltpu.VMEM((SRC, TOK, D), BF),
            pltpu.VMEM((SRC, 16, TOK), F32),
            pltpu.VMEM((TOK, ROUTED), F32),
            pltpu.VMEM((TOK, ROUTED), F32),
            pltpu.VMEM((ROWS, D), BF),
            pltpu.VMEM((D, ROWS), BF),
            pltpu.VMEM((ROWS, D), BF),
            pltpu.VMEM((ROWS, FF), BF),
            pltpu.VMEM((FF, ROWS), BF),
            pltpu.VMEM((ROWS, 2 * FF), BF),
            pltpu.VMEM((D, 2 * FF), BF),
            pltpu.VMEM((FF, D), BF),
            pltpu.VMEM((RING, 2, 16, 128, 128), BF),
            pltpu.VMEM((DEP, 2, 6, 2, 128, 128), BF),
            pltpu.VMEM((DEP, 2, 6, 64, 128), BF),
            pltpu.VMEM((ROWS, D), BF),
            pltpu.VMEM((ROWS, D), BF),
            pltpu.VMEM((ROWS, TOK), BF),
            pltpu.VMEM((ROWS, 1), F32),
            pltpu.VMEM((SRC, 8, TOK), F32),
            pltpu.VMEM((SRC, 8, TOK), F32),
            dma((4,)),
            dma((2, 14)), dma((2, SRC, 2)),
            dma((SRC,)), dma((SRC,)),
            dma((SRC,)), dma((SRC,)),
            dma((SRC,)), dma((SRC,)),
            dma((DEP, 2, 6)), dma((DEP, 2, 6)),
            dma((DEP, 2, 6)), dma((DEP, 2, 6)),
        ],
        compiler_params=pltpu.CompilerParams(
            collective_id=0, has_side_effects=True, vmem_limit_bytes=67043328
        ),
        name="moe_backward",
    )(
        tokens, out_grad, z_weight.reshape(1, TOK), router_weight, expert_ids,
        gate_up_weight[0], down_weight[0],
    )
    router_part = lax.dot_general(
        tokens, logit_grad, (((0,), (0,)), ((), ())), preferred_element_type=F32
    )
    router_grad = lax.psum(router_part, ("dp", "expert"))
    return token_grad, router_grad, gate_up_grad[None], down_grad[None]


def solution(mesh):
    return jax.shard_map(
        per_device,
        mesh=mesh,
        in_specs=(
            P(("dp", "expert"), None),
            P(("dp", "expert"), None),
            P(("dp", "expert")),
            P(),
            P(("dp", "expert"), None),
            P("expert", None, None),
            P("expert", None, None),
        ),
        out_specs=(
            P(("dp", "expert"), None),
            P(),
            P("expert", "dp", None),
            P("expert", "dp", None),
        ),
        check_vma=False,
    )
```

```python
import functools

import jax
import jax.numpy as jnp
from jax import lax
from jax.experimental import pallas as pl
from jax.experimental.pallas import tpu as pltpu
from jax.sharding import PartitionSpec as P

BF = jnp.bfloat16
F32 = jnp.float32
MESH = pl.DeviceIdType.MESH

TOK = 128
CAP = 64
D = 2048
FF = 1536
SRC = 8
NDP = 16
ROWS = SRC * CAP
ROUTED = 128
ND = D // 256
NG = 2 * FF // 256
NC = ND + NG
LAG1, LAG2, LAG3, LAG4 = 1, 3, 4, 6
DEP = 6
RING = 7
INV = (0, 1, 4, 5, 2, 3, 6, 7)


def nt(a, b):
    return lax.dot_general(a, b, (((1,), (1,)), ((), ())), preferred_element_type=F32)


def tn(a, b):
    return lax.dot_general(a, b, (((0,), (0,)), ((), ())), preferred_element_type=F32)


def nn(a, b):
    return jnp.dot(a, b, preferred_element_type=F32)


def kernel(
    tokens_hbm, grad_hbm, z_ref, rw_ref, ids_ref, gu_hbm, dn_hbm,
    tg_out, rt_out, gug_out, dng_out,
    xa, oa, meta, prob, logit, xr, xt, dy, hid, hidt, pg, gu, dn,
    part, r1, r2, rg, rb, sel, psum, psend, precv, lgrad, rpart, rin, rsum, rbuf,
    lsem, ag_s, ag_r, mt_s, mt_r, ps_s, ps_r, rt_s, rt_r, s1, q1, s2, q2, ra_s, ra_r, rs_s, rs_r, rc_s, rc_r, rd_s, rd_r,
):
    dp = lax.axis_index("dp")
    ex = lax.axis_index("expert")
    px, pz = dp // 4, dp % 4
    py, pc = ex // 2, ex % 2
    xp, xm = ((px + 1) % 4) * 4 + pz, ((px + 3) % 4) * 4 + pz
    zp, zm = px * 4 + (pz + 1) % 4, px * 4 + (pz + 3) % 4
    yp, ym, yo = (py + 1) % 4, (py + 3) % 4, (py + 2) % 4
    oc = 1 - pc
    place = (ex, py * 2 + oc, ym * 2 + pc, ym * 2 + oc, yp * 2 + pc, yp * 2 + oc, yo * 2 + pc, yo * 2 + oc)

    cp_tok = pltpu.make_async_copy(tokens_hbm, xa.at[0], lsem.at[0])
    cp_grad = pltpu.make_async_copy(grad_hbm, oa.at[0], lsem.at[1])
    cp_gu = pltpu.make_async_copy(gu_hbm, gu, lsem.at[2])
    cp_dn = pltpu.make_async_copy(dn_hbm, dn, lsem.at[3])
    cp_tok.start()
    cp_grad.start()
    cp_gu.start()
    cp_dn.start()

    barrier = pltpu.get_barrier_semaphore()
    for k in range(1, NDP):
        pl.semaphore_signal(barrier, inc=1, device_id=((dp + k) % NDP, ex), device_id_type=MESH)
    for q in range(1, SRC):
        pl.semaphore_signal(barrier, inc=1, device_id=(dp, place[q]), device_id_type=MESH)
    pl.semaphore_wait(barrier, NDP - 1 + SRC - 1)

    def ag(arr, buf, src_q, half, to_q, dst_q, k):
        rows = pl.ds(half * CAP, CAP)
        return pltpu.make_async_remote_copy(
            src_ref=buf.at[src_q, rows], dst_ref=buf.at[dst_q, rows],
            send_sem=ag_s.at[arr, k], recv_sem=ag_r.at[arr, dst_q, half],
            device_id=(dp, place[to_q]), device_id_type=MESH,
        )

    def ag_wait(arr, buf, q, half):
        rows = pl.ds(half * CAP, CAP)
        pltpu.make_async_remote_copy(
            src_ref=buf.at[q, rows], dst_ref=buf.at[q, rows],
            send_sem=ag_s.at[arr, 0], recv_sem=ag_r.at[arr, q, half],
            device_id=(dp, place[1]), device_id_type=MESH,
        ).wait_recv()

    def ag_own(arr, buf):
        out = [
            ag(arr, buf, 0, 0, 4, 2, 0), ag(arr, buf, 0, 1, 2, 4, 1),
            ag(arr, buf, 0, 1, 4, 2, 2), ag(arr, buf, 0, 0, 2, 4, 3),
            ag(arr, buf, 0, 0, 1, 1, 4), ag(arr, buf, 0, 1, 1, 1, 5),
        ]
        for c in out:
            c.start()
        return out

    def ag_relay(arr, buf):
        ag_wait(arr, buf, 2, 0)
        a = ag(arr, buf, 2, 0, 4, 6, 6)
        a.start()
        b = ag(arr, buf, 2, 0, 1, 3, 8)
        b.start()
        ag_wait(arr, buf, 4, 1)
        c = ag(arr, buf, 4, 1, 2, 6, 7)
        c.start()
        d = ag(arr, buf, 4, 1, 1, 5, 9)
        d.start()
        return [a, b, c, d]

    def ag_near(arr, buf):
        ag_wait(arr, buf, 2, 1)
        a = ag(arr, buf, 2, 1, 1, 3, 10)
        a.start()
        ag_wait(arr, buf, 4, 0)
        b = ag(arr, buf, 4, 0, 1, 5, 11)
        b.start()
        return [a, b]

    def ag_far(arr, buf):
        out = []
        for half in range(2):
            ag_wait(arr, buf, 6, half)
            a = ag(arr, buf, 6, half, 1, 7, 12 + half)
            a.start()
            out.append(a)
        return out

    def ag_side(arr, buf, q):
        ag_wait(arr, buf, q, 0)
        ag_wait(arr, buf, q, 1)

    sent = []
    cp_tok.wait()
    sent += ag_own(0, xa)

    sub = lax.broadcasted_iota(jnp.int32, (TOK, TOK), 0)
    lane = lax.broadcasted_iota(jnp.int32, (TOK, TOK), 1)
    lg = nn(xa[0], rw_ref[...])
    logit[...] = lg
    ids = ids_ref[...].astype(F32)
    ids = jnp.concatenate([ids, ids], axis=0).T
    lane_f = lane.astype(F32)
    dense = jnp.zeros((TOK, ROUTED), F32)
    mask = jnp.zeros((TOK, ROUTED), F32)
    total = jnp.zeros((TOK, 1), F32)
    for k in range(4):
        hit = ids[:, k : k + 1] == lane_f
        value = jnp.exp(jnp.sum(jnp.where(hit, lg, 0.0), axis=1, keepdims=True))
        total = total + value
        dense = jnp.where(hit, value, dense)
        mask = jnp.where(hit, 1.0, mask)
    dense = dense / total
    prob[...] = dense
    before = jnp.where(lane < sub, 1.0, 0.0).astype(BF)
    rank = nn(before, mask.astype(BF))
    rank = jnp.where(mask > 0.5, rank, -1.0)
    meta[0, 0:8, :] = dense.T[0:8]
    meta[0, 8:16, :] = rank.T[0:8]
    meta_sent = []
    for q in range(1, SRC):
        c = pltpu.make_async_remote_copy(
            src_ref=meta.at[0], dst_ref=meta.at[INV[q]], send_sem=mt_s.at[q], recv_sem=mt_r.at[INV[q]],
            device_id=(dp, place[q]), device_id_type=MESH,
        )
        c.start()
        meta_sent.append(c)

    sent += ag_relay(0, xa)
    cp_grad.wait()
    sent += ag_own(1, oa)
    sent += ag_near(0, xa)

    for q in range(1, SRC):
        pltpu.make_async_remote_copy(
            src_ref=meta.at[0], dst_ref=meta.at[q], send_sem=mt_s.at[q], recv_sem=mt_r.at[q],
            device_id=(dp, place[q]), device_id_type=MESH,
        ).wait_recv()

    slot_of = lax.broadcasted_iota(jnp.int32, (CAP, TOK), 0).astype(F32)

    def pick(q):
        return (slot_of == meta[q, pl.ds(8 + ex, 1), :]).astype(F32)

    def gather_tok(q):
        rows = nn(pick(q).astype(BF), xa[q]).astype(BF)
        xr[q * CAP : (q + 1) * CAP, :] = rows

    def gather_grad(q):
        p = pick(q)
        weight = jnp.sum(p * meta[q, pl.ds(ex, 1), :], axis=1, keepdims=True)
        rows = nn(p.astype(BF), oa[q])
        dy[q * CAP : (q + 1) * CAP, :] = (weight * rows).astype(BF)

    for q in (1, 3, 5):
        ag_side(0, xa, q)
    for q in range(6):
        gather_tok(q)
    sent += ag_far(0, xa)
    gather_tok(6)
    ag_side(0, xa, 7)
    gather_tok(7)
    cp_gu.wait()

    def forward(f, _):
        a = pl.ds(pl.multiple_of(f * 256, 256), 256)
        b = pl.ds(pl.multiple_of(FF + f * 256, 256), 256)
        g = nn(xr[...], gu[:, a])
        u = nn(xr[...], gu[:, b])
        s = lax.logistic(g)
        act = g * s
        h = (act * u).astype(BF)
        hid[:, a] = h
        hidt[a, :] = h.T
        pg[:, a] = (u * s * (1.0 + g * (1.0 - s))).astype(BF)
        pg[:, b] = act.astype(BF)
        return 0

    lax.fori_loop(0, 3, forward, 0)
    sent += ag_relay(1, oa)
    lax.fori_loop(3, 6, forward, 0)
    sent += ag_near(1, oa)

    def flip(k, _):
        a = pl.ds(pl.multiple_of(k * 256, 256), 256)
        xt[a, :] = xr[:, a].T
        return 0

    lax.fori_loop(0, D // 256, flip, 0)
    for q in (1, 3, 5):
        ag_side(1, oa, q)
    for q in range(6):
        gather_grad(q)
    sent += ag_far(1, oa)
    gather_grad(6)
    ag_side(1, oa, 7)
    gather_grad(7)
    cp_dn.wait()
    for c in sent:
        c.wait_send()
    for c in meta_sent:
        c.wait_send()

    axes = (((xp, xm, px), (zp, zm, pz)), ((zp, zm, pz), (xp, xm, px)))

    def send1(col, kind, slot, ring, zr):
        plus, minus, fc = axes[col][0]
        base = (
            ((fc + 2) % 4) * 4, ((fc + 2) % 4) * 4 + 2,
            ((fc + 1) % 4) * 4 + 2, ((fc + 3) % 4) * 4,
            ((fc + 1) % 4) * 4, ((fc + 3) % 4) * 4 + 2,
        )[kind]
        return pltpu.make_async_remote_copy(
            src_ref=part.at[ring, col, pl.ds(base, 2), pl.ds(0, zr)],
            dst_ref=r1.at[slot, col, kind, :, pl.ds(0, zr)],
            send_sem=s1.at[slot, col, kind], recv_sem=q1.at[slot, col, kind],
            device_id=(plus if kind % 2 == 0 else minus, ex), device_id_type=MESH,
        )

    def send2(col, kind, slot, ring, zr):
        plus, minus, sc = axes[col][1]
        fc = axes[col][0][2]
        h = zr // 2
        step, low = ((2, 0), (2, h), (1, h), (3, 0), (1, 0), (3, h))[kind]
        return pltpu.make_async_remote_copy(
            src_ref=part.at[ring, col, fc * 4 + (sc + step) % 4, pl.ds(low, h)],
            dst_ref=r2.at[slot, col, kind, pl.ds(0, h)],
            send_sem=s2.at[slot, col, kind], recv_sem=q2.at[slot, col, kind],
            device_id=(plus if kind % 2 == 0 else minus, ex), device_id_type=MESH,
        )

    def f32(v):
        return v.astype(F32)

    def compute(c, lhs, rhs_of, zr):
        slot, ring = c % DEP, c % RING
        rhs = rhs_of(c)
        rows = 4 * zr

        def one(b, _):
            r = nn(lhs[pl.ds(pl.multiple_of(b * rows, rows), rows), :], rhs).astype(BF)
            for k in range(4):
                part[ring, 0, b * 4 + k, 0:zr] = r[k * zr : (k + 1) * zr, 0:128]
                part[ring, 1, k * 4 + b, 0:zr] = r[k * zr : (k + 1) * zr, 128:256]
            return 0

        lax.fori_loop(0, 4, one, 0)
        for kind in range(4):
            for col in range(2):
                send1(col, kind, slot, ring, zr).start()

    def stage1(c, zr):
        slot, ring = c % DEP, c % RING
        for col in range(2):
            fc = axes[col][0][2]
            for kind in range(2):
                send1(col, kind, slot, ring, zr).wait_recv()
                base = ((fc + 1) % 4) * 4 if kind == 0 else ((fc + 3) % 4) * 4 + 2
                at = (ring, col, pl.ds(base, 2), pl.ds(0, zr))
                part[at] = (f32(part[at]) + f32(r1[slot, col, kind, :, 0:zr])).astype(BF)
                send1(col, 4 + kind, slot, ring, zr).start()

    def stage2(c, zr):
        slot, ring = c % DEP, c % RING
        for col in range(2):
            fc = axes[col][0][2]
            for kind in range(2, 6):
                send1(col, kind, slot, ring, zr).wait_recv()
            for half, (a, b) in enumerate(((4, 3), (2, 5))):
                at = (ring, col, pl.ds(fc * 4 + 2 * half, 2), pl.ds(0, zr))
                part[at] = (
                    f32(part[at]) + f32(r1[slot, col, a, :, 0:zr]) + f32(r1[slot, col, b, :, 0:zr])
                ).astype(BF)
            for kind in range(4):
                send1(col, kind, slot, ring, zr).wait_send()
            for kind in range(4):
                send2(col, kind, slot, ring, zr).start()

    def stage3(c, zr):
        slot, ring = c % DEP, c % RING
        h = zr // 2
        for col in range(2):
            fc, sc = axes[col][0][2], axes[col][1][2]
            for kind in range(2):
                send2(col, kind, slot, ring, zr).wait_recv()
                step, low = ((1, 0), (3, h))[kind]
                at = (ring, col, fc * 4 + (sc + step) % 4, pl.ds(low, h))
                part[at] = (f32(part[at]) + f32(r2[slot, col, kind, 0:h])).astype(BF)
                send2(col, 4 + kind, slot, ring, zr).start()
            for kind in range(4, 6):
                send1(col, kind, slot, ring, zr).wait_send()

    def stage4(c, zr, out, first):
        slot, ring = c % DEP, c % RING
        h = zr // 2
        for col in range(2):
            fc, sc = axes[col][0][2], axes[col][1][2]
            for kind in range(2, 6):
                send2(col, kind, slot, ring, zr).wait_recv()
            cols = pl.ds(pl.multiple_of((c - first) * 256 + col * 128, 128), 128)
            for half, (a, b) in enumerate(((4, 3), (2, 5))):
                own = part[ring, col, fc * 4 + sc, half * h : (half + 1) * h]
                out[half * h : (half + 1) * h, cols] = (
                    f32(own) + f32(r2[slot, col, a, 0:h]) + f32(r2[slot, col, b, 0:h])
                ).astype(BF)
            for kind in range(6):
                send2(col, kind, slot, ring, zr).wait_send()

    def both(c, fn, on_down, on_gate):
        @pl.when(jnp.logical_and(c >= 0, c < ND))
        def _():
            fn(c, *on_down)

        @pl.when(jnp.logical_and(c >= ND, c < NC))
        def _():
            fn(c, *on_gate)

    ZD, ZG = FF // 16, D // 16

    def down_rhs(c):
        return dy[:, pl.ds(pl.multiple_of(c * 256, 256), 256)]

    def gate_rhs(c):
        return pg[:, pl.ds(pl.multiple_of((c - ND) * 256, 256), 256)]

    def hidden_grad(f):
        a = pl.ds(pl.multiple_of(f * 256, 256), 256)
        b = pl.ds(pl.multiple_of(FF + f * 256, 256), 256)
        hg = nt(dy[...], dn[a, :])
        score = jnp.sum(f32(hid[:, a]) * hg, axis=1, keepdims=True)
        psum[...] = jnp.where(f == 0, 0.0, psum[...]) + score
        pg[:, a] = (f32(pg[:, a]) * hg).astype(BF)
        pg[:, b] = (f32(pg[:, b]) * hg).astype(BF)

    def ps_copy(q):
        return pltpu.make_async_remote_copy(
            src_ref=psend.at[q], dst_ref=precv.at[INV[q]], send_sem=ps_s.at[q], recv_sem=ps_r.at[INV[q]],
            device_id=(dp, place[q]), device_id_type=MESH,
        )

    def send_scores():
        for q in range(SRC):
            row = jnp.sum(pick(q) * psum[q * CAP : (q + 1) * CAP, :], axis=0, keepdims=True)
            if q == 0:
                precv[0] = jnp.broadcast_to(row, (8, TOK))
            else:
                psend[q] = jnp.broadcast_to(row, (8, TOK))
        for q in range(1, SRC):
            ps_copy(q).start()

    def row_grad(k):
        def one(j, _):
            at = pl.ds(pl.multiple_of((k * 2 + j) * 256, 256), 256)
            rg[:, at] = nt(pg[...], gu[at, :]).astype(BF)
            return 0

        lax.fori_loop(0, 2, one, 0)

    def rt_copy(q):
        return pltpu.make_async_remote_copy(
            src_ref=rg.at[pl.ds(q * CAP, CAP)], dst_ref=rb.at[pl.ds(INV[q] * CAP, CAP)],
            send_sem=rt_s.at[q], recv_sem=rt_r.at[INV[q]],
            device_id=(dp, place[q]), device_id_type=MESH,
        )

    def rt_wait(q):
        pltpu.make_async_remote_copy(
            src_ref=rg.at[pl.ds(q * CAP, CAP)], dst_ref=rb.at[pl.ds(q * CAP, CAP)],
            send_sem=rt_s.at[q], recv_sem=rt_r.at[q],
            device_id=(dp, place[q]), device_id_type=MESH,
        ).wait_recv()

    def send_rows():
        for q in range(1, SRC):
            rt_copy(q).start()
        rb[0:CAP, :] = rg[0:CAP, :]

    def logit_grad():
        for q in range(1, SRC):
            pltpu.make_async_remote_copy(
                src_ref=psend.at[q], dst_ref=precv.at[q], send_sem=ps_s.at[q], recv_sem=ps_r.at[q],
                device_id=(dp, place[q]), device_id_type=MESH,
            ).wait_recv()
        for q in range(1, SRC):
            ps_copy(q).wait_send()
        scores = jnp.zeros((ROUTED, TOK), F32)
        for q in range(SRC):
            scores = jnp.where(sub == place[q], precv[q, 0:1, :], scores)
        scores = scores.T
        mean = jnp.sum(scores, axis=1, keepdims=True)
        z = jnp.sum(jnp.where(sub == lane, z_ref[...], 0.0), axis=1, keepdims=True)
        lgt = logit[...]
        log_total = jnp.log(jnp.sum(jnp.exp(lgt), axis=1, keepdims=True))
        z_grad = 2.0 * z * log_total * jnp.exp(lgt - log_total)
        lgrad[...] = (z_grad + scores - prob[...] * mean).astype(BF)

    def token_grad():
        for q in range(1, SRC):
            rt_wait(q)
        for q in range(1, SRC):
            rt_copy(q).wait_send()
        for q in range(SRC):
            sel[q * CAP : (q + 1) * CAP, :] = (
                slot_of == meta[0, pl.ds(8 + place[q], 1), :]
            ).astype(F32).astype(BF)
        chosen = sel[...]
        grad = lgrad[...]

        def one(k, _):
            at = pl.ds(pl.multiple_of(k * 256, 256), 256)
            tg_out[:, at] = (tn(chosen, rb[:, at]) + nt(grad, rw_ref[at, :])).astype(BF)
            return 0

        lax.fori_loop(0, D // 256, one, 0)

    def ra_copy(q):
        return pltpu.make_async_remote_copy(
            src_ref=rpart.at[place[q]], dst_ref=rin.at[INV[q]], send_sem=ra_s.at[q], recv_sem=ra_r.at[INV[q]],
            device_id=(dp, place[q]), device_id_type=MESH,
        )

    def ra_wait(q):
        pltpu.make_async_remote_copy(
            src_ref=rpart.at[place[q]], dst_ref=rin.at[q], send_sem=ra_s.at[q], recv_sem=ra_r.at[q],
            device_id=(dp, place[q]), device_id_type=MESH,
        ).wait_recv()

    def rs_copy(k):
        to = (dp + k) % NDP
        return pltpu.make_async_remote_copy(
            src_ref=rsum.at[to], dst_ref=rbuf.at[k], send_sem=rs_s.at[k], recv_sem=rs_r.at[k],
            device_id=(to, ex), device_id_type=MESH,
        )

    def rc_copy(k):
        to = (dp + k) % NDP
        return pltpu.make_async_remote_copy(
            src_ref=rt_out.at[ex, dp], dst_ref=rt_out.at[ex, dp], send_sem=rc_s.at[k], recv_sem=rc_r.at[k],
            device_id=(to, ex), device_id_type=MESH,
        )

    def rc_wait(k):
        fr = (dp + NDP - k) % NDP
        pltpu.make_async_remote_copy(
            src_ref=rt_out.at[ex, fr], dst_ref=rt_out.at[ex, fr], send_sem=rc_s.at[k], recv_sem=rc_r.at[k],
            device_id=(fr, ex), device_id_type=MESH,
        ).wait_recv()

    def rd_copy(q):
        return pltpu.make_async_remote_copy(
            src_ref=rt_out.at[ex], dst_ref=rt_out.at[ex], send_sem=rd_s.at[q], recv_sem=rd_r.at[INV[q]],
            device_id=(dp, place[q]), device_id_type=MESH,
        )

    def rd_wait(q):
        pltpu.make_async_remote_copy(
            src_ref=rt_out.at[place[q]], dst_ref=rt_out.at[place[q]], send_sem=rd_s.at[q], recv_sem=rd_r.at[q],
            device_id=(dp, place[q]), device_id_type=MESH,
        ).wait_recv()

    def router_a():
        grad = lgrad[...]

        def one(b, _):
            at = pl.ds(pl.multiple_of(b * 256, 256), 256)
            rpart[b] = tn(xa[0, :, at], grad)
            return 0

        lax.fori_loop(0, SRC, one, 0)
        for q in range(1, SRC):
            ra_copy(q).start()

    def router_b():
        for q in range(1, SRC):
            ra_wait(q)
        acc = rpart[ex]
        for q in range(1, SRC):
            acc = acc + rin[q]
        rsum[...] = acc.reshape(NDP, 16, ROUTED)
        for k in range(1, NDP):
            rs_copy(k).start()

    def router_c():
        acc = rsum[dp]
        for k in range(1, NDP):
            rs_copy(k).wait_recv()
            acc = acc + rbuf[k]
        rt_out[ex, dp] = acc
        for k in range(1, NDP):
            rc_copy(k).start()

    def router_d():
        for k in range(1, NDP):
            rc_wait(k)
        for q in range(1, SRC):
            rd_copy(q).start()

    def router_end():
        for q in range(1, SRC):
            rd_wait(q)
        for q in range(1, SRC):
            ra_copy(q).wait_send()
            rd_copy(q).wait_send()
        for k in range(1, NDP):
            rs_copy(k).wait_send()
            rc_copy(k).wait_send()

    def body(i, _):
        @pl.when(i < ND)
        def _():
            compute(i, hidt, down_rhs, ZD)

        @pl.when(jnp.logical_and(i >= ND, i < NC))
        def _():
            compute(i, xt, gate_rhs, ZG)

        @pl.when(i < 6)
        def _():
            hidden_grad(i)

        @pl.when(i == 6)
        def _():
            send_scores()

        @pl.when(jnp.logical_and(i >= ND, i < ND + 4))
        def _():
            row_grad(i - ND)

        @pl.when(i == ND + 3)
        def _():
            send_rows()

        for at, step in (
            (ND, logit_grad), (ND, router_a), (ND + 4, router_b), (ND + 6, router_c),
            (ND + 8, router_d), (NC + 1, router_end),
        ):
            pl.when(i == at)(step)

        @pl.when(i == NC)
        def _():
            token_grad()

        c4 = i - LAG4

        @pl.when(jnp.logical_and(c4 >= 0, c4 < ND))
        def _():
            stage4(c4, ZD, dng_out, 0)

        @pl.when(c4 >= ND)
        def _():
            stage4(c4, ZG, gug_out, ND)

        both(i - LAG3, stage3, (ZD,), (ZG,))
        both(i - LAG2, stage2, (ZD,), (ZG,))
        both(i - LAG1, stage1, (ZD,), (ZG,))
        return 0

    lax.fori_loop(0, NC + LAG4, body, 0)


def write_out(*refs):
    sem = refs[8]
    copies = [pltpu.make_async_copy(refs[k], refs[4 + k], sem.at[k]) for k in range(4)]
    for c in copies:
        c.start()
    for c in copies:
        c.wait()


def per_device(tokens, out_grad, z_weight, router_weight, expert_ids, gate_up_weight, down_weight):
    vmem = pl.BlockSpec(memory_space=pltpu.VMEM)
    hbm = pl.BlockSpec(memory_space=pl.ANY)
    dma = pltpu.SemaphoreType.DMA
    outs = pl.pallas_call(
        kernel,
        out_shape=(
            jax.ShapeDtypeStruct((TOK, D), BF),
            jax.ShapeDtypeStruct((SRC, NDP, 16, ROUTED), F32),
            jax.ShapeDtypeStruct((D // 16, 2 * FF), BF),
            jax.ShapeDtypeStruct((FF // 16, D), BF),
        ),
        in_specs=[hbm, hbm, vmem, vmem, vmem, hbm, hbm],
        out_specs=(vmem, vmem, vmem, vmem),
        scratch_shapes=[
            pltpu.VMEM((SRC, TOK, D), BF),
            pltpu.VMEM((SRC, TOK, D), BF),
            pltpu.VMEM((SRC, 16, TOK), F32),
            pltpu.VMEM((TOK, ROUTED), F32),
            pltpu.VMEM((TOK, ROUTED), F32),
            pltpu.VMEM((ROWS, D), BF),
            pltpu.VMEM((D, ROWS), BF),
            pltpu.VMEM((ROWS, D), BF),
            pltpu.VMEM((ROWS, FF), BF),
            pltpu.VMEM((FF, ROWS), BF),
            pltpu.VMEM((ROWS, 2 * FF), BF),
            pltpu.VMEM((D, 2 * FF), BF),
            pltpu.VMEM((FF, D), BF),
            pltpu.VMEM((RING, 2, 16, 128, 128), BF),
            pltpu.VMEM((DEP, 2, 6, 2, 128, 128), BF),
            pltpu.VMEM((DEP, 2, 6, 64, 128), BF),
            pltpu.VMEM((ROWS, D), BF),
            pltpu.VMEM((ROWS, D), BF),
            pltpu.VMEM((ROWS, TOK), BF),
            pltpu.VMEM((ROWS, 1), F32),
            pltpu.VMEM((SRC, 8, TOK), F32),
            pltpu.VMEM((SRC, 8, TOK), F32),
            pltpu.VMEM((TOK, ROUTED), BF),
            pltpu.VMEM((SRC, D // SRC, ROUTED), F32),
            pltpu.VMEM((SRC, D // SRC, ROUTED), F32),
            pltpu.VMEM((NDP, 16, ROUTED), F32),
            pltpu.VMEM((NDP, 16, ROUTED), F32),
            dma((4,)),
            dma((2, 14)), dma((2, SRC, 2)),
            dma((SRC,)), dma((SRC,)),
            dma((SRC,)), dma((SRC,)),
            dma((SRC,)), dma((SRC,)),
            dma((DEP, 2, 6)), dma((DEP, 2, 6)),
            dma((DEP, 2, 6)), dma((DEP, 2, 6)),
            dma((SRC,)), dma((SRC,)),
            dma((NDP,)), dma((NDP,)),
            dma((NDP,)), dma((NDP,)),
            dma((SRC,)), dma((SRC,)),
        ],
        compiler_params=pltpu.CompilerParams(
            collective_id=0, has_side_effects=True, vmem_limit_bytes=67043328
        ),
        name="moe_backward",
    )(
        tokens, out_grad, z_weight.reshape(1, TOK), router_weight, expert_ids.T,
        gate_up_weight[0], down_weight[0],
    )
    shapes = tuple(jax.ShapeDtypeStruct(o.shape, o.dtype) for o in outs)
    token_grad, router_grad, gate_up_grad, down_grad = pl.pallas_call(
        write_out,
        out_shape=shapes,
        in_specs=[vmem] * 4,
        out_specs=[hbm] * 4,
        scratch_shapes=[dma((4,))],
        name="write_out",
    )(*outs)
    return token_grad, router_grad.reshape(D, ROUTED), gate_up_grad[None], down_grad[None]


def solution(mesh):
    return jax.shard_map(
        per_device,
        mesh=mesh,
        in_specs=(
            P(("dp", "expert"), None),
            P(("dp", "expert"), None),
            P(("dp", "expert")),
            P(),
            P(("dp", "expert"), None),
            P("expert", None, None),
            P("expert", None, None),
        ),
        out_specs=(
            P(("dp", "expert"), None),
            P(),
            P("expert", "dp", None),
            P("expert", "dp", None),
        ),
        check_vma=False,
    )
```

```python
import functools

import jax
import jax.numpy as jnp
from jax import lax
from jax.experimental import pallas as pl
from jax.experimental.pallas import tpu as pltpu
from jax.sharding import PartitionSpec as P

BF = jnp.bfloat16
F32 = jnp.float32
MESH = pl.DeviceIdType.MESH

TOK = 128
CAP = 64
D = 2048
FF = 1536
SRC = 8
NDP = 16
ROWS = SRC * CAP
ROUTED = 128
ND = D // 256
NG = 2 * FF // 256
NC = ND + NG
LAG1, LAG2, LAG3, LAG4 = 1, 3, 4, 6
DEP = 6
RING = 7
CUTS = (0, 256, 512, 1024, 1536, 2048)
INV = (0, 1, 4, 5, 2, 3, 6, 7)


def nt(a, b):
    return lax.dot_general(a, b, (((1,), (1,)), ((), ())), preferred_element_type=F32)


def tn(a, b):
    return lax.dot_general(a, b, (((0,), (0,)), ((), ())), preferred_element_type=F32)


def nn(a, b):
    return jnp.dot(a, b, preferred_element_type=F32)


def kernel(
    tokens_hbm, grad_hbm, z_ref, rw_ref, ids_ref, gu_hbm, dn_hbm,
    tg_out, rt_out, gug_out, dng_out,
    xa, oa, meta, prob, logit, xr, xt, dy, hid, hidt, pg, gu, dn,
    part, r1, r2, rg, rb, sel, psum, psend, precv, lgrad, rpart, rin, rsum, rbufz, rsumx, rbufx,
    lsem, ag_s, ag_r, mt_s, mt_r, ps_s, ps_r, rt_s, rt_r, s1, q1, s2, q2, ra_s, ra_r, rs_s, rs_r, rd_s, rd_r,
):
    dp = lax.axis_index("dp")
    ex = lax.axis_index("expert")
    px, pz = dp // 4, dp % 4
    py, pc = ex // 2, ex % 2

    def xs(k):
        return ((px + k) % 4) * 4 + pz

    def zs(k):
        return px * 4 + (pz + k) % 4

    xp, xm, zp, zm = xs(1), xs(3), zs(1), zs(3)
    yp, ym, yo = (py + 1) % 4, (py + 3) % 4, (py + 2) % 4
    oc = 1 - pc
    place = (ex, py * 2 + oc, ym * 2 + pc, ym * 2 + oc, yp * 2 + pc, yp * 2 + oc, yo * 2 + pc, yo * 2 + oc)

    cp_tok = pltpu.make_async_copy(tokens_hbm, xa.at[0], lsem.at[0])
    cp_grad = pltpu.make_async_copy(grad_hbm, oa.at[0], lsem.at[1])
    cp_gu = pltpu.make_async_copy(gu_hbm, gu, lsem.at[2])
    cp_dn = pltpu.make_async_copy(dn_hbm, dn, lsem.at[3])
    cp_tok.start()
    cp_grad.start()
    cp_gu.start()
    cp_dn.start()

    barrier = pltpu.get_barrier_semaphore()
    for k in range(1, 4):
        pl.semaphore_signal(barrier, inc=1, device_id=(xs(k), ex), device_id_type=MESH)
        pl.semaphore_signal(barrier, inc=1, device_id=(zs(k), ex), device_id_type=MESH)
    for q in range(1, SRC):
        pl.semaphore_signal(barrier, inc=1, device_id=(dp, place[q]), device_id_type=MESH)
    pl.semaphore_wait(barrier, 6 + SRC - 1)

    OWN = ((0, 0, 4, 2), (0, 1, 2, 4), (0, 1, 4, 2), (0, 0, 2, 4), (0, 0, 1, 1), (0, 1, 1, 1))
    RELAY = ((2, 0, 4, 6), (2, 0, 1, 3), (4, 1, 2, 6), (4, 1, 1, 5))
    NEAR = ((2, 1, 1, 3), (4, 0, 1, 5))
    FAR = ((6, 0, 1, 7), (6, 1, 1, 7))
    ALL = OWN + RELAY + NEAR + FAR

    def ag_view(part_no, q, half):
        rows = pl.ds(half * CAP, CAP)
        if part_no == 0:
            return xa.at[q, rows]
        return oa.at[q, rows, pl.ds(CUTS[part_no - 1], CUTS[part_no] - CUTS[part_no - 1])]

    def ag(part_no, copy):
        src_q, half, to_q, dst_q = copy
        return pltpu.make_async_remote_copy(
            src_ref=ag_view(part_no, src_q, half), dst_ref=ag_view(part_no, dst_q, half),
            send_sem=ag_s.at[part_no, ALL.index(copy)], recv_sem=ag_r.at[part_no, dst_q, half],
            device_id=(dp, place[to_q]), device_id_type=MESH,
        )

    def ag_wait(part_no, q, half):
        pltpu.make_async_remote_copy(
            src_ref=ag_view(part_no, q, half), dst_ref=ag_view(part_no, q, half),
            send_sem=ag_s.at[part_no, 0], recv_sem=ag_r.at[part_no, q, half],
            device_id=(dp, place[1]), device_id_type=MESH,
        ).wait_recv()

    def ag_own(part_no):
        for c in OWN:
            ag(part_no, c).start()

    def ag_relay(part_no):
        ag_wait(part_no, 2, 0)
        ag(part_no, RELAY[0]).start()
        ag(part_no, RELAY[1]).start()
        ag_wait(part_no, 4, 1)
        ag(part_no, RELAY[2]).start()
        ag(part_no, RELAY[3]).start()

    def ag_near(part_no):
        ag_wait(part_no, 2, 1)
        ag(part_no, NEAR[0]).start()
        ag_wait(part_no, 4, 0)
        ag(part_no, NEAR[1]).start()

    def ag_far(part_no):
        for half in range(2):
            ag_wait(part_no, 6, half)
            ag(part_no, FAR[half]).start()

    def ag_side(part_no, q):
        ag_wait(part_no, q, 0)
        ag_wait(part_no, q, 1)

    cp_tok.wait()
    ag_own(0)

    sub = lax.broadcasted_iota(jnp.int32, (TOK, TOK), 0)
    lane = lax.broadcasted_iota(jnp.int32, (TOK, TOK), 1)
    lg = nn(xa[0], rw_ref[...])
    logit[...] = lg
    ids = ids_ref[...].astype(F32)
    ids = jnp.concatenate([ids, ids], axis=0).T
    lane_f = lane.astype(F32)
    dense = jnp.zeros((TOK, ROUTED), F32)
    mask = jnp.zeros((TOK, ROUTED), F32)
    total = jnp.zeros((TOK, 1), F32)
    for k in range(4):
        hit = ids[:, k : k + 1] == lane_f
        value = jnp.exp(jnp.sum(jnp.where(hit, lg, 0.0), axis=1, keepdims=True))
        total = total + value
        dense = jnp.where(hit, value, dense)
        mask = jnp.where(hit, 1.0, mask)
    dense = dense / total
    prob[...] = dense
    before = jnp.where(lane < sub, 1.0, 0.0).astype(BF)
    rank = nn(before, mask.astype(BF))
    rank = jnp.where(mask > 0.5, rank, -1.0)
    meta[0, 0:8, :] = dense.T[0:8]
    meta[0, 8:16, :] = rank.T[0:8]
    meta_sent = []
    for q in range(1, SRC):
        c = pltpu.make_async_remote_copy(
            src_ref=meta.at[0], dst_ref=meta.at[INV[q]], send_sem=mt_s.at[q], recv_sem=mt_r.at[INV[q]],
            device_id=(dp, place[q]), device_id_type=MESH,
        )
        c.start()
        meta_sent.append(c)

    cp_grad.wait()
    ag_own(1)
    ag_relay(0)
    ag_own(2)
    ag_near(0)

    for q in range(1, SRC):
        pltpu.make_async_remote_copy(
            src_ref=meta.at[0], dst_ref=meta.at[q], send_sem=mt_s.at[q], recv_sem=mt_r.at[q],
            device_id=(dp, place[q]), device_id_type=MESH,
        ).wait_recv()

    slot_of = lax.broadcasted_iota(jnp.int32, (CAP, TOK), 0).astype(F32)

    def pick(q):
        return (slot_of == meta[q, pl.ds(8 + ex, 1), :]).astype(F32)

    def gather_tok(q):
        rows = nn(pick(q).astype(BF), xa[q]).astype(BF)
        xr[q * CAP : (q + 1) * CAP, :] = rows

    def gather_grad(q, part_no):
        p = pick(q)
        weight = jnp.sum(p * meta[q, pl.ds(ex, 1), :], axis=1, keepdims=True)
        cols = slice(CUTS[part_no - 1], CUTS[part_no])
        rows = nn(p.astype(BF), oa[q, :, cols])
        dy[q * CAP : (q + 1) * CAP, cols] = (weight * rows).astype(BF)

    def grad_near(part_no):
        for q in (1, 3, 5):
            ag_side(part_no, q)
        for q in range(6):
            gather_grad(q, part_no)

    def grad_far(part_no):
        ag_far(part_no)
        gather_grad(6, part_no)
        ag_side(part_no, 7)
        gather_grad(7, part_no)

    def grad_part(part_no):
        grad_near(part_no)
        grad_far(part_no)

    def forward(lo, hi):
        def run(f, _):
            a = pl.ds(pl.multiple_of(f * 256, 256), 256)
            b = pl.ds(pl.multiple_of(FF + f * 256, 256), 256)
            g = nn(xr[lo:hi, :], gu[:, a])
            u = nn(xr[lo:hi, :], gu[:, b])
            s = lax.logistic(g)
            act = g * s
            h = (act * u).astype(BF)
            hid[lo:hi, a] = h
            hidt[a, lo:hi] = h.T
            pg[lo:hi, a] = (u * s * (1.0 + g * (1.0 - s))).astype(BF)
            pg[lo:hi, b] = act.astype(BF)
            return 0

        return run

    near, far = forward(0, 6 * CAP), forward(6 * CAP, ROWS)
    for q in (1, 3, 5):
        ag_side(0, q)
    for q in range(6):
        gather_tok(q)
    cp_gu.wait()
    lax.fori_loop(0, 6, near, 0)
    ag_relay(1)
    ag_own(3)
    ag_far(0)
    gather_tok(6)
    ag_near(1)
    ag_side(0, 7)
    gather_tok(7)
    lax.fori_loop(0, 3, far, 0)
    ag_relay(2)
    lax.fori_loop(3, 6, far, 0)
    ag_near(2)
    grad_part(1)
    cp_dn.wait()

    def flip(k):
        a = pl.ds(pl.multiple_of(k * 256, 256), 256)
        xt[a, :] = xr[:, a].T

    axes = (((xp, xm, px), (zp, zm, pz)), ((zp, zm, pz), (xp, xm, px)))

    def send1(col, kind, slot, ring, zr):
        plus, minus, fc = axes[col][0]
        base = (
            ((fc + 2) % 4) * 4, ((fc + 2) % 4) * 4 + 2,
            ((fc + 1) % 4) * 4 + 2, ((fc + 3) % 4) * 4,
            ((fc + 1) % 4) * 4, ((fc + 3) % 4) * 4 + 2,
        )[kind]
        return pltpu.make_async_remote_copy(
            src_ref=part.at[ring, col, pl.ds(base, 2), pl.ds(0, zr)],
            dst_ref=r1.at[slot, col, kind, :, pl.ds(0, zr)],
            send_sem=s1.at[slot, col, kind], recv_sem=q1.at[slot, col, kind],
            device_id=(plus if kind % 2 == 0 else minus, ex), device_id_type=MESH,
        )

    def send2(col, kind, slot, ring, zr):
        plus, minus, sc = axes[col][1]
        fc = axes[col][0][2]
        h = zr // 2
        step, low = ((2, 0), (2, h), (1, h), (3, 0), (1, 0), (3, h))[kind]
        return pltpu.make_async_remote_copy(
            src_ref=part.at[ring, col, fc * 4 + (sc + step) % 4, pl.ds(low, h)],
            dst_ref=r2.at[slot, col, kind, pl.ds(0, h)],
            send_sem=s2.at[slot, col, kind], recv_sem=q2.at[slot, col, kind],
            device_id=(plus if kind % 2 == 0 else minus, ex), device_id_type=MESH,
        )

    def f32(v):
        return v.astype(F32)

    def compute(c, lhs, rhs_of, zr):
        slot, ring = c % DEP, c % RING
        rhs = rhs_of(c)
        rows = 4 * zr

        def one(b, _):
            r = nn(lhs[pl.ds(pl.multiple_of(b * rows, rows), rows), :], rhs).astype(BF)
            for k in range(4):
                part[ring, 0, b * 4 + k, 0:zr] = r[k * zr : (k + 1) * zr, 0:128]
                part[ring, 1, k * 4 + b, 0:zr] = r[k * zr : (k + 1) * zr, 128:256]
            return 0

        lax.fori_loop(0, 4, one, 0)
        for kind in range(4):
            for col in range(2):
                send1(col, kind, slot, ring, zr).start()

    def stage1(c, zr):
        slot, ring = c % DEP, c % RING
        for col in range(2):
            fc = axes[col][0][2]
            for kind in range(2):
                send1(col, kind, slot, ring, zr).wait_recv()
                base = ((fc + 1) % 4) * 4 if kind == 0 else ((fc + 3) % 4) * 4 + 2
                at = (ring, col, pl.ds(base, 2), pl.ds(0, zr))
                part[at] = (f32(part[at]) + f32(r1[slot, col, kind, :, 0:zr])).astype(BF)
                send1(col, 4 + kind, slot, ring, zr).start()

    def stage2(c, zr):
        slot, ring = c % DEP, c % RING
        for col in range(2):
            fc = axes[col][0][2]
            for kind in range(2, 6):
                send1(col, kind, slot, ring, zr).wait_recv()
            for half, (a, b) in enumerate(((4, 3), (2, 5))):
                at = (ring, col, pl.ds(fc * 4 + 2 * half, 2), pl.ds(0, zr))
                part[at] = (
                    f32(part[at]) + f32(r1[slot, col, a, :, 0:zr]) + f32(r1[slot, col, b, :, 0:zr])
                ).astype(BF)
            for kind in range(4):
                send1(col, kind, slot, ring, zr).wait_send()
            for kind in range(4):
                send2(col, kind, slot, ring, zr).start()

    def stage3(c, zr):
        slot, ring = c % DEP, c % RING
        h = zr // 2
        for col in range(2):
            fc, sc = axes[col][0][2], axes[col][1][2]
            for kind in range(2):
                send2(col, kind, slot, ring, zr).wait_recv()
                step, low = ((1, 0), (3, h))[kind]
                at = (ring, col, fc * 4 + (sc + step) % 4, pl.ds(low, h))
                part[at] = (f32(part[at]) + f32(r2[slot, col, kind, 0:h])).astype(BF)
                send2(col, 4 + kind, slot, ring, zr).start()
            for kind in range(4, 6):
                send1(col, kind, slot, ring, zr).wait_send()

    def stage4(c, zr, out, first):
        slot, ring = c % DEP, c % RING
        h = zr // 2
        for col in range(2):
            fc, sc = axes[col][0][2], axes[col][1][2]
            for kind in range(2, 6):
                send2(col, kind, slot, ring, zr).wait_recv()
            cols = pl.ds(pl.multiple_of((c - first) * 256 + col * 128, 128), 128)
            for half, (a, b) in enumerate(((4, 3), (2, 5))):
                own = part[ring, col, fc * 4 + sc, half * h : (half + 1) * h]
                out[half * h : (half + 1) * h, cols] = (
                    f32(own) + f32(r2[slot, col, a, 0:h]) + f32(r2[slot, col, b, 0:h])
                ).astype(BF)
            for kind in range(6):
                send2(col, kind, slot, ring, zr).wait_send()

    def both(c, fn, on_down, on_gate):
        @pl.when(jnp.logical_and(c >= 0, c < ND))
        def _():
            fn(c, *on_down)

        @pl.when(jnp.logical_and(c >= ND, c < NC))
        def _():
            fn(c, *on_gate)

    ZD, ZG = FF // 16, D // 16

    def down_rhs(c):
        return dy[:, pl.ds(pl.multiple_of(c * 256, 256), 256)]

    def gate_rhs(c):
        return pg[:, pl.ds(pl.multiple_of((c - ND) * 256, 256), 256)]

    def hidden_grad(f):
        a = pl.ds(pl.multiple_of(f * 256, 256), 256)
        b = pl.ds(pl.multiple_of(FF + f * 256, 256), 256)
        hg = nt(dy[...], dn[a, :])
        score = jnp.sum(f32(hid[:, a]) * hg, axis=1, keepdims=True)
        psum[...] = jnp.where(f == 0, 0.0, psum[...]) + score
        pg[:, a] = (f32(pg[:, a]) * hg).astype(BF)
        pg[:, b] = (f32(pg[:, b]) * hg).astype(BF)

    def ps_copy(q):
        return pltpu.make_async_remote_copy(
            src_ref=psend.at[q], dst_ref=precv.at[INV[q]], send_sem=ps_s.at[q], recv_sem=ps_r.at[INV[q]],
            device_id=(dp, place[q]), device_id_type=MESH,
        )

    def send_scores():
        for q in range(SRC):
            row = jnp.sum(pick(q) * psum[q * CAP : (q + 1) * CAP, :], axis=0, keepdims=True)
            if q == 0:
                precv[0] = jnp.broadcast_to(row, (8, TOK))
            else:
                psend[q] = jnp.broadcast_to(row, (8, TOK))
        for q in range(1, SRC):
            ps_copy(q).start()

    def row_grad(k):
        at = pl.ds(pl.multiple_of(k * 256, 256), 256)
        rg[:, at] = nt(pg[...], gu[at, :]).astype(BF)

    HALF = D // 2

    def rt_copy(q, half):
        cols = pl.ds(half * HALF, HALF)
        return pltpu.make_async_remote_copy(
            src_ref=rg.at[pl.ds(q * CAP, CAP), cols], dst_ref=rb.at[pl.ds(INV[q] * CAP, CAP), cols],
            send_sem=rt_s.at[half, q], recv_sem=rt_r.at[half, INV[q]],
            device_id=(dp, place[q]), device_id_type=MESH,
        )

    def rt_wait(q, half):
        cols = pl.ds(half * HALF, HALF)
        pltpu.make_async_remote_copy(
            src_ref=rg.at[pl.ds(q * CAP, CAP), cols], dst_ref=rb.at[pl.ds(q * CAP, CAP), cols],
            send_sem=rt_s.at[half, q], recv_sem=rt_r.at[half, q],
            device_id=(dp, place[q]), device_id_type=MESH,
        ).wait_recv()

    def send_rows(half):
        for q in range(1, SRC):
            rt_copy(q, half).start()
        cols = slice(half * HALF, (half + 1) * HALF)
        rb[0:CAP, cols] = rg[0:CAP, cols]

    def logit_grad():
        for q in range(1, SRC):
            pltpu.make_async_remote_copy(
                src_ref=psend.at[q], dst_ref=precv.at[q], send_sem=ps_s.at[q], recv_sem=ps_r.at[q],
                device_id=(dp, place[q]), device_id_type=MESH,
            ).wait_recv()
        for q in range(1, SRC):
            ps_copy(q).wait_send()
        scores = jnp.zeros((ROUTED, TOK), F32)
        for q in range(SRC):
            scores = jnp.where(sub == place[q], precv[q, 0:1, :], scores)
        scores = scores.T
        mean = jnp.sum(scores, axis=1, keepdims=True)
        z = jnp.sum(jnp.where(sub == lane, z_ref[...], 0.0), axis=1, keepdims=True)
        lgt = logit[...]
        log_total = jnp.log(jnp.sum(jnp.exp(lgt), axis=1, keepdims=True))
        z_grad = 2.0 * z * log_total * jnp.exp(lgt - log_total)
        lgrad[...] = (z_grad + scores - prob[...] * mean).astype(BF)

    def token_grad(half):
        for q in range(1, SRC):
            rt_wait(q, half)
        for q in range(1, SRC):
            rt_copy(q, half).wait_send()
        if half == 0:
            for q in range(SRC):
                sel[q * CAP : (q + 1) * CAP, :] = (
                    slot_of == meta[0, pl.ds(8 + place[q], 1), :]
                ).astype(F32).astype(BF)
        chosen = sel[...]
        grad = lgrad[...]

        def one(k, _):
            at = pl.ds(pl.multiple_of(k * 256, 256), 256)
            tg_out[:, at] = (tn(chosen, rb[:, at]) + nt(grad, rw_ref[at, :])).astype(BF)
            return 0

        lax.fori_loop(half * 4, half * 4 + 4, one, 0)

    def ra_copy(q):
        return pltpu.make_async_remote_copy(
            src_ref=rpart.at[place[q]], dst_ref=rin.at[INV[q]], send_sem=ra_s.at[q], recv_sem=ra_r.at[INV[q]],
            device_id=(dp, place[q]), device_id_type=MESH,
        )

    def ra_wait(q):
        pltpu.make_async_remote_copy(
            src_ref=rpart.at[place[q]], dst_ref=rin.at[q], send_sem=ra_s.at[q], recv_sem=ra_r.at[q],
            device_id=(dp, place[q]), device_id_type=MESH,
        ).wait_recv()

    c1, c2 = pz + pc * (px - pz), px + pc * (pz - px)

    def to1(k):
        return zs(k) + pc * (xs(k) - zs(k))

    def to2(k):
        return xs(k) + pc * (zs(k) - xs(k))

    def rsz(k):
        return pltpu.make_async_remote_copy(
            src_ref=rsum.at[:, (c1 + k) % 4], dst_ref=rbufz.at[k], send_sem=rs_s.at[0, k], recv_sem=rs_r.at[0, k],
            device_id=(to1(k), ex), device_id_type=MESH,
        )

    def rsx(k):
        return pltpu.make_async_remote_copy(
            src_ref=rsumx.at[(c2 + k) % 4], dst_ref=rbufx.at[k], send_sem=rs_s.at[1, k], recv_sem=rs_r.at[1, k],
            device_id=(to2(k), ex), device_id_type=MESH,
        )

    def rcx(k, at):
        block = rt_out.at[ex, at, c1]
        return pltpu.make_async_remote_copy(
            src_ref=block, dst_ref=block, send_sem=rs_s.at[2, k], recv_sem=rs_r.at[2, k],
            device_id=(to2(k), ex), device_id_type=MESH,
        )

    def rcz(k, at):
        block = rt_out.at[ex, :, at]
        return pltpu.make_async_remote_copy(
            src_ref=block, dst_ref=block, send_sem=rs_s.at[3, k], recv_sem=rs_r.at[3, k],
            device_id=(to1(k), ex), device_id_type=MESH,
        )

    SAME = (2, 4, 6)

    def rd_copy(q, to_q):
        block = rt_out.at[place[q]]
        return pltpu.make_async_remote_copy(
            src_ref=block, dst_ref=block, send_sem=rd_s.at[q, to_q],
            recv_sem=rd_r.at[INV[to_q] if to_q != 1 else q + 1],
            device_id=(dp, place[to_q]), device_id_type=MESH,
        )

    def rd_wait(q):
        block = rt_out.at[place[q]]
        pltpu.make_async_remote_copy(
            src_ref=block, dst_ref=block, send_sem=rd_s.at[0, 1], recv_sem=rd_r.at[q],
            device_id=(dp, place[1]), device_id_type=MESH,
        ).wait_recv()

    def router_a():
        grad = lgrad[...]

        def one(b, _):
            at = pl.ds(pl.multiple_of(b * 256, 256), 256)
            rpart[b] = tn(xa[0, :, at], grad).astype(BF)
            return 0

        lax.fori_loop(0, SRC, one, 0)
        for q in range(1, SRC):
            ra_copy(q).start()

    def router_b():
        for q in range(1, SRC):
            ra_wait(q)
        acc = f32(rpart[ex])
        for q in range(1, SRC):
            acc = acc + f32(rin[q])
        rsum[...] = acc.reshape(4, 4, 16, ROUTED).astype(BF)
        for k in range(1, 4):
            rsz(k).start()

    def router_c():
        acc = f32(rsum[:, c1])
        for k in range(1, 4):
            rsz(k).wait_recv()
            acc = acc + f32(rbufz[k])
        rsumx[...] = acc.astype(BF)
        for k in range(1, 4):
            rsx(k).start()

    def router_x():
        acc = f32(rsumx[c2])
        for k in range(1, 4):
            rsx(k).wait_recv()
            acc = acc + f32(rbufx[k])
        rt_out[ex, c2, c1] = acc
        for k in range(1, 4):
            rcx(k, c2).start()

    def router_z():
        for k in range(1, 4):
            rcx(k, (c2 + 4 - k) % 4).wait_recv()
        for k in range(1, 4):
            rcz(k, c1).start()

    def router_d():
        for k in range(1, 4):
            rcz(k, (c1 + 4 - k) % 4).wait_recv()
        for to_q in SAME:
            rd_copy(0, to_q).start()
        rd_copy(0, 1).start()

    def router_e():
        for q in SAME:
            rd_wait(q)
            rd_copy(q, 1).start()

    def router_end():
        for q in (1, 3, 5, 7):
            rd_wait(q)
        for q in range(1, SRC):
            ra_copy(q).wait_send()
        for to_q in SAME:
            rd_copy(0, to_q).wait_send()
        for q in (0,) + SAME:
            rd_copy(q, 1).wait_send()
        for k in range(1, 4):
            rsz(k).wait_send()
            rsx(k).wait_send()
            rcx(k, c2).wait_send()
            rcz(k, c1).wait_send()

    def body(i, _):
        @pl.when(i < ND)
        def _():
            compute(i, hidt, down_rhs, ZD)

        @pl.when(jnp.logical_and(i >= ND, i < NC))
        def _():
            compute(i, xt, gate_rhs, ZG)

        def parts(k):
            if k == 0:
                ag_relay(3)
                ag_own(4)
                grad_part(2)
            elif k == 1:
                ag_near(3)
                grad_part(3)
                ag_relay(4)
                ag_own(5)
            elif k == 2:
                ag_near(4)
            elif k == 3:
                grad_part(4)
                ag_relay(5)
            elif k == 4:
                ag_near(5)
                grad_part(5)
            else:
                for n in range(6):
                    for c in ALL:
                        ag(n, c).wait_send()
                for c in meta_sent:
                    c.wait_send()

        for k in range(6):
            pl.when(i == k)(functools.partial(parts, k))

        @pl.when(jnp.logical_and(i >= 5, i < 8))
        def _():
            hidden_grad(2 * i - 10)
            hidden_grad(2 * i - 9)

        @pl.when(i < 8)
        def _():
            flip(i)

        @pl.when(i == 7)
        def _():
            send_scores()

        @pl.when(jnp.logical_and(i >= ND, i < ND + 4))
        def _():
            row_grad(2 * (i - ND))
            row_grad(2 * (i - ND) + 1)

        for at, step in (
            (ND, logit_grad), (ND, router_a), (ND + 4, router_b), (ND + 5, router_c),
            (ND + 6, router_x), (ND + 7, router_z), (ND + 8, router_d), (NC - 1, router_e), (NC + 1, router_end),
            (ND + 1, functools.partial(send_rows, 0)), (ND + 3, functools.partial(send_rows, 1)),
            (NC - 3, functools.partial(token_grad, 0)), (NC - 1, functools.partial(token_grad, 1)),
        ):
            pl.when(i == at)(step)

        c4 = i - LAG4

        @pl.when(jnp.logical_and(c4 >= 0, c4 < ND))
        def _():
            stage4(c4, ZD, dng_out, 0)

        @pl.when(c4 >= ND)
        def _():
            stage4(c4, ZG, gug_out, ND)

        both(i - LAG3, stage3, (ZD,), (ZG,))
        both(i - LAG2, stage2, (ZD,), (ZG,))
        both(i - LAG1, stage1, (ZD,), (ZG,))
        return 0

    lax.fori_loop(0, NC + LAG4, body, 0)


def write_out(*refs):
    sem = refs[8]
    copies = [pltpu.make_async_copy(refs[k], refs[4 + k], sem.at[k]) for k in range(4)]
    for c in copies:
        c.start()
    for c in copies:
        c.wait()


def per_device(tokens, out_grad, z_weight, router_weight, expert_ids, gate_up_weight, down_weight):
    vmem = pl.BlockSpec(memory_space=pltpu.VMEM)
    hbm = pl.BlockSpec(memory_space=pl.ANY)
    dma = pltpu.SemaphoreType.DMA
    outs = pl.pallas_call(
        kernel,
        out_shape=(
            jax.ShapeDtypeStruct((TOK, D), BF),
            jax.ShapeDtypeStruct((SRC, 4, 4, 16, ROUTED), F32),
            jax.ShapeDtypeStruct((D // 16, 2 * FF), BF),
            jax.ShapeDtypeStruct((FF // 16, D), BF),
        ),
        in_specs=[hbm, hbm, vmem, vmem, vmem, hbm, hbm],
        out_specs=(vmem, vmem, vmem, vmem),
        scratch_shapes=[
            pltpu.VMEM((SRC, TOK, D), BF),
            pltpu.VMEM((SRC, TOK, D), BF),
            pltpu.VMEM((SRC, 16, TOK), F32),
            pltpu.VMEM((TOK, ROUTED), F32),
            pltpu.VMEM((TOK, ROUTED), F32),
            pltpu.VMEM((ROWS, D), BF),
            pltpu.VMEM((D, ROWS), BF),
            pltpu.VMEM((ROWS, D), BF),
            pltpu.VMEM((ROWS, FF), BF),
            pltpu.VMEM((FF, ROWS), BF),
            pltpu.VMEM((ROWS, 2 * FF), BF),
            pltpu.VMEM((D, 2 * FF), BF),
            pltpu.VMEM((FF, D), BF),
            pltpu.VMEM((RING, 2, 16, 128, 128), BF),
            pltpu.VMEM((DEP, 2, 6, 2, 128, 128), BF),
            pltpu.VMEM((DEP, 2, 6, 64, 128), BF),
            pltpu.VMEM((ROWS, D), BF),
            pltpu.VMEM((ROWS, D), BF),
            pltpu.VMEM((ROWS, TOK), BF),
            pltpu.VMEM((ROWS, 1), F32),
            pltpu.VMEM((SRC, 8, TOK), F32),
            pltpu.VMEM((SRC, 8, TOK), F32),
            pltpu.VMEM((TOK, ROUTED), BF),
            pltpu.VMEM((SRC, D // SRC, ROUTED), BF),
            pltpu.VMEM((SRC, D // SRC, ROUTED), BF),
            pltpu.VMEM((4, 4, 16, ROUTED), BF),
            pltpu.VMEM((4, 4, 16, ROUTED), BF),
            pltpu.VMEM((4, 16, ROUTED), BF),
            pltpu.VMEM((4, 16, ROUTED), BF),
            dma((4,)),
            dma((6, 14)), dma((6, SRC, 2)),
            dma((SRC,)), dma((SRC,)),
            dma((SRC,)), dma((SRC,)),
            dma((2, SRC)), dma((2, SRC)),
            dma((DEP, 2, 6)), dma((DEP, 2, 6)),
            dma((DEP, 2, 6)), dma((DEP, 2, 6)),
            dma((SRC,)), dma((SRC,)),
            dma((4, 4)), dma((4, 4)),
            dma((SRC, SRC)), dma((SRC,)),
        ],
        compiler_params=pltpu.CompilerParams(
            collective_id=0, has_side_effects=True, vmem_limit_bytes=67043328
        ),
        name="moe_backward",
    )(
        tokens, out_grad, z_weight.reshape(1, TOK), router_weight, expert_ids.T,
        gate_up_weight[0], down_weight[0],
    )
    shapes = tuple(jax.ShapeDtypeStruct(o.shape, o.dtype) for o in outs)
    token_grad, router_grad, gate_up_grad, down_grad = pl.pallas_call(
        write_out,
        out_shape=shapes,
        in_specs=[vmem] * 4,
        out_specs=[hbm] * 4,
        scratch_shapes=[dma((4,))],
        name="write_out",
    )(*outs)
    return token_grad, router_grad.reshape(D, ROUTED), gate_up_grad[None], down_grad[None]


def solution(mesh):
    return jax.shard_map(
        per_device,
        mesh=mesh,
        in_specs=(
            P(("dp", "expert"), None),
            P(("dp", "expert"), None),
            P(("dp", "expert")),
            P(),
            P(("dp", "expert"), None),
            P("expert", None, None),
            P("expert", None, None),
        ),
        out_specs=(
            P(("dp", "expert"), None),
            P(),
            P("expert", "dp", None),
            P("expert", "dp", None),
        ),
        check_vma=False,
    )
```

```python
import functools

import jax
import jax.numpy as jnp
from jax import lax
from jax.experimental import pallas as pl
from jax.experimental.pallas import tpu as pltpu
from jax.sharding import PartitionSpec as P

BF = jnp.bfloat16
F32 = jnp.float32
MESH = pl.DeviceIdType.MESH

TOK = 128
CAP = 64
D = 2048
FF = 1536
SRC = 8
NDP = 16
ROWS = SRC * CAP
ROUTED = 128
ND = D // 256
NG = 2 * FF // 256
NC = ND + NG
LAG1, LAG2, LAG3, LAG4 = 1, 3, 4, 6
DEP = 6
RING = 7
CUTS = (0, 256, 512, 1024, 1536, 2048)
INV = (0, 1, 4, 5, 2, 3, 6, 7)


def nt(a, b):
    return lax.dot_general(a, b, (((1,), (1,)), ((), ())), preferred_element_type=F32)


def tn(a, b):
    return lax.dot_general(a, b, (((0,), (0,)), ((), ())), preferred_element_type=F32)


def nn(a, b):
    return jnp.dot(a, b, preferred_element_type=F32)


def kernel(
    tokens_hbm, grad_hbm, z_hbm, rw_hbm, ids_hbm, gu_hbm, dn_hbm,
    tg_hbm, rt_hbm, gug_hbm, dng_hbm,
    z_ref, rw_ref, ids_ref, tg_out, rt_out, gug_out, dng_out,
    xa, oa, meta, prob, logit, xr, xt, dy, hid, hidt, pg, gu, dn,
    part, r1, r2, rg, rb, sel, psum, psend, precv, lgrad, rpart, rin, rsum, rbufz, rsumx, rbufx,
    lsem, osem, ag_s, ag_r, mt_s, mt_r, ps_s, ps_r, rt_s, rt_r, s1, q1, s2, q2, ra_s, ra_r, rs_s, rs_r, rd_s, rd_r,
):
    dp = lax.axis_index("dp")
    ex = lax.axis_index("expert")
    px, pz = dp // 4, dp % 4
    py, pc = ex // 2, ex % 2

    def xs(k):
        return ((px + k) % 4) * 4 + pz

    def zs(k):
        return px * 4 + (pz + k) % 4

    xp, xm, zp, zm = xs(1), xs(3), zs(1), zs(3)
    yp, ym, yo = (py + 1) % 4, (py + 3) % 4, (py + 2) % 4
    oc = 1 - pc
    place = (ex, py * 2 + oc, ym * 2 + pc, ym * 2 + oc, yp * 2 + pc, yp * 2 + oc, yo * 2 + pc, yo * 2 + oc)

    cp_tok = pltpu.make_async_copy(tokens_hbm, xa.at[0], lsem.at[0])
    cp_grad = pltpu.make_async_copy(grad_hbm, oa.at[0], lsem.at[1])
    cp_gu = pltpu.make_async_copy(gu_hbm, gu, lsem.at[2])
    cp_dn = pltpu.make_async_copy(dn_hbm, dn, lsem.at[3])
    cp_rw = pltpu.make_async_copy(rw_hbm, rw_ref, lsem.at[4])
    cp_z = pltpu.make_async_copy(z_hbm, z_ref, lsem.at[5])
    cp_ids = pltpu.make_async_copy(ids_hbm, ids_ref, lsem.at[6])
    cp_tok.start()

    barrier = pltpu.get_barrier_semaphore()
    for k in range(1, 4):
        pl.semaphore_signal(barrier, inc=1, device_id=(xs(k), ex), device_id_type=MESH)
        pl.semaphore_signal(barrier, inc=1, device_id=(zs(k), ex), device_id_type=MESH)
    for q in range(1, SRC):
        pl.semaphore_signal(barrier, inc=1, device_id=(dp, place[q]), device_id_type=MESH)
    cp_rw.start()
    cp_ids.start()
    cp_z.start()
    cp_grad.start()
    cp_gu.start()
    cp_dn.start()
    pl.semaphore_wait(barrier, 6 + SRC - 1)

    OWN = ((0, 0, 4, 2), (0, 1, 2, 4), (0, 1, 4, 2), (0, 0, 2, 4), (0, 0, 1, 1), (0, 1, 1, 1))
    RELAY = ((2, 0, 4, 6), (2, 0, 1, 3), (4, 1, 2, 6), (4, 1, 1, 5))
    NEAR = ((2, 1, 1, 3), (4, 0, 1, 5))
    FAR = ((6, 0, 1, 7), (6, 1, 1, 7))
    ALL = OWN + RELAY + NEAR + FAR

    def ag_view(part_no, q, half):
        rows = pl.ds(half * CAP, CAP)
        if part_no == 0:
            return xa.at[q, rows]
        return oa.at[q, rows, pl.ds(CUTS[part_no - 1], CUTS[part_no] - CUTS[part_no - 1])]

    def ag(part_no, copy):
        src_q, half, to_q, dst_q = copy
        return pltpu.make_async_remote_copy(
            src_ref=ag_view(part_no, src_q, half), dst_ref=ag_view(part_no, dst_q, half),
            send_sem=ag_s.at[part_no, ALL.index(copy)], recv_sem=ag_r.at[part_no, dst_q, half],
            device_id=(dp, place[to_q]), device_id_type=MESH,
        )

    def ag_wait(part_no, q, half):
        pltpu.make_async_remote_copy(
            src_ref=ag_view(part_no, q, half), dst_ref=ag_view(part_no, q, half),
            send_sem=ag_s.at[part_no, 0], recv_sem=ag_r.at[part_no, q, half],
            device_id=(dp, place[1]), device_id_type=MESH,
        ).wait_recv()

    def ag_own(part_no):
        for c in OWN:
            ag(part_no, c).start()

    def ag_relay(part_no):
        ag_wait(part_no, 2, 0)
        ag(part_no, RELAY[0]).start()
        ag(part_no, RELAY[1]).start()
        ag_wait(part_no, 4, 1)
        ag(part_no, RELAY[2]).start()
        ag(part_no, RELAY[3]).start()

    def ag_near(part_no):
        ag_wait(part_no, 2, 1)
        ag(part_no, NEAR[0]).start()
        ag_wait(part_no, 4, 0)
        ag(part_no, NEAR[1]).start()

    def ag_far(part_no):
        for half in range(2):
            ag_wait(part_no, 6, half)
            ag(part_no, FAR[half]).start()

    def ag_side(part_no, q):
        ag_wait(part_no, q, 0)
        ag_wait(part_no, q, 1)

    cp_tok.wait()
    ag_own(0)

    sub = lax.broadcasted_iota(jnp.int32, (TOK, TOK), 0)
    lane = lax.broadcasted_iota(jnp.int32, (TOK, TOK), 1)
    cp_rw.wait()
    cp_ids.wait()
    cp_z.wait()
    lg = nn(xa[0], rw_ref[...])
    logit[...] = lg
    ids = ids_ref[...].astype(F32)
    ids = jnp.concatenate([ids, ids], axis=0).T
    lane_f = lane.astype(F32)
    dense = jnp.zeros((TOK, ROUTED), F32)
    mask = jnp.zeros((TOK, ROUTED), F32)
    total = jnp.zeros((TOK, 1), F32)
    for k in range(4):
        hit = ids[:, k : k + 1] == lane_f
        value = jnp.exp(jnp.sum(jnp.where(hit, lg, 0.0), axis=1, keepdims=True))
        total = total + value
        dense = jnp.where(hit, value, dense)
        mask = jnp.where(hit, 1.0, mask)
    dense = dense / total
    prob[...] = dense
    before = jnp.where(lane < sub, 1.0, 0.0).astype(BF)
    rank = nn(before, mask.astype(BF))
    rank = jnp.where(mask > 0.5, rank, -1.0)
    meta[0, 0:8, :] = dense.T[0:8]
    meta[0, 8:16, :] = rank.T[0:8]
    meta_sent = []
    for q in range(1, SRC):
        c = pltpu.make_async_remote_copy(
            src_ref=meta.at[0], dst_ref=meta.at[INV[q]], send_sem=mt_s.at[q], recv_sem=mt_r.at[INV[q]],
            device_id=(dp, place[q]), device_id_type=MESH,
        )
        c.start()
        meta_sent.append(c)

    cp_grad.wait()
    ag_own(1)
    ag_relay(0)
    ag_own(2)
    ag_near(0)

    for q in range(1, SRC):
        pltpu.make_async_remote_copy(
            src_ref=meta.at[0], dst_ref=meta.at[q], send_sem=mt_s.at[q], recv_sem=mt_r.at[q],
            device_id=(dp, place[q]), device_id_type=MESH,
        ).wait_recv()

    slot_of = lax.broadcasted_iota(jnp.int32, (CAP, TOK), 0).astype(F32)

    def pick(q):
        return (slot_of == meta[q, pl.ds(8 + ex, 1), :]).astype(F32)

    def gather_tok(q):
        rows = nn(pick(q).astype(BF), xa[q]).astype(BF)
        xr[q * CAP : (q + 1) * CAP, :] = rows

    def gather_grad(q, part_no):
        p = pick(q)
        weight = jnp.sum(p * meta[q, pl.ds(ex, 1), :], axis=1, keepdims=True)
        cols = slice(CUTS[part_no - 1], CUTS[part_no])
        rows = nn(p.astype(BF), oa[q, :, cols])
        dy[q * CAP : (q + 1) * CAP, cols] = (weight * rows).astype(BF)

    def grad_near(part_no):
        for q in (1, 3, 5):
            ag_side(part_no, q)
        for q in range(6):
            gather_grad(q, part_no)

    def grad_far(part_no):
        ag_far(part_no)
        gather_grad(6, part_no)
        ag_side(part_no, 7)
        gather_grad(7, part_no)

    def grad_part(part_no):
        grad_near(part_no)
        grad_far(part_no)

    def forward(lo, hi):
        def run(f, _):
            a = pl.ds(pl.multiple_of(f * 256, 256), 256)
            b = pl.ds(pl.multiple_of(FF + f * 256, 256), 256)
            g = nn(xr[lo:hi, :], gu[:, a])
            u = nn(xr[lo:hi, :], gu[:, b])
            s = lax.logistic(g)
            act = g * s
            h = (act * u).astype(BF)
            hid[lo:hi, a] = h
            hidt[a, lo:hi] = h.T
            pg[lo:hi, a] = (u * s * (1.0 + g * (1.0 - s))).astype(BF)
            pg[lo:hi, b] = act.astype(BF)
            return 0

        return run

    near, far = forward(0, 6 * CAP), forward(6 * CAP, ROWS)
    for q in (1, 3, 5):
        ag_side(0, q)
    for q in range(6):
        gather_tok(q)
    cp_gu.wait()
    lax.fori_loop(0, 6, near, 0)
    ag_relay(1)
    ag_own(3)
    ag_far(0)
    gather_tok(6)
    ag_near(1)
    ag_side(0, 7)
    gather_tok(7)
    lax.fori_loop(0, 3, far, 0)
    ag_relay(2)
    lax.fori_loop(3, 6, far, 0)
    ag_near(2)
    grad_part(1)
    cp_dn.wait()

    def flip(k):
        a = pl.ds(pl.multiple_of(k * 256, 256), 256)
        xt[a, :] = xr[:, a].T

    axes = (((xp, xm, px), (zp, zm, pz)), ((zp, zm, pz), (xp, xm, px)))

    def send1(col, kind, slot, ring, zr):
        plus, minus, fc = axes[col][0]
        base = (
            ((fc + 2) % 4) * 4, ((fc + 2) % 4) * 4 + 2,
            ((fc + 1) % 4) * 4 + 2, ((fc + 3) % 4) * 4,
            ((fc + 1) % 4) * 4, ((fc + 3) % 4) * 4 + 2,
        )[kind]
        return pltpu.make_async_remote_copy(
            src_ref=part.at[ring, col, pl.ds(base, 2), pl.ds(0, zr)],
            dst_ref=r1.at[slot, col, kind, :, pl.ds(0, zr)],
            send_sem=s1.at[slot, col, kind], recv_sem=q1.at[slot, col, kind],
            device_id=(plus if kind % 2 == 0 else minus, ex), device_id_type=MESH,
        )

    def send2(col, kind, slot, ring, zr):
        plus, minus, sc = axes[col][1]
        fc = axes[col][0][2]
        h = zr // 2
        step, low = ((2, 0), (2, h), (1, h), (3, 0), (1, 0), (3, h))[kind]
        return pltpu.make_async_remote_copy(
            src_ref=part.at[ring, col, fc * 4 + (sc + step) % 4, pl.ds(low, h)],
            dst_ref=r2.at[slot, col, kind, pl.ds(0, h)],
            send_sem=s2.at[slot, col, kind], recv_sem=q2.at[slot, col, kind],
            device_id=(plus if kind % 2 == 0 else minus, ex), device_id_type=MESH,
        )

    def f32(v):
        return v.astype(F32)

    def compute(c, lhs, rhs_of, zr):
        slot, ring = c % DEP, c % RING
        rhs = rhs_of(c)
        rows = 4 * zr

        def one(b, _):
            r = nn(lhs[pl.ds(pl.multiple_of(b * rows, rows), rows), :], rhs).astype(BF)
            for k in range(4):
                part[ring, 0, b * 4 + k, 0:zr] = r[k * zr : (k + 1) * zr, 0:128]
                part[ring, 1, k * 4 + b, 0:zr] = r[k * zr : (k + 1) * zr, 128:256]
            return 0

        lax.fori_loop(0, 4, one, 0)
        for kind in range(4):
            for col in range(2):
                send1(col, kind, slot, ring, zr).start()

    def stage1(c, zr):
        slot, ring = c % DEP, c % RING
        for col in range(2):
            fc = axes[col][0][2]
            for kind in range(2):
                send1(col, kind, slot, ring, zr).wait_recv()
                base = ((fc + 1) % 4) * 4 if kind == 0 else ((fc + 3) % 4) * 4 + 2
                at = (ring, col, pl.ds(base, 2), pl.ds(0, zr))
                part[at] = (f32(part[at]) + f32(r1[slot, col, kind, :, 0:zr])).astype(BF)
                send1(col, 4 + kind, slot, ring, zr).start()

    def stage2(c, zr):
        slot, ring = c % DEP, c % RING
        for col in range(2):
            fc = axes[col][0][2]
            for kind in range(2, 6):
                send1(col, kind, slot, ring, zr).wait_recv()
            for half, (a, b) in enumerate(((4, 3), (2, 5))):
                at = (ring, col, pl.ds(fc * 4 + 2 * half, 2), pl.ds(0, zr))
                part[at] = (
                    f32(part[at]) + f32(r1[slot, col, a, :, 0:zr]) + f32(r1[slot, col, b, :, 0:zr])
                ).astype(BF)
            for kind in range(4):
                send1(col, kind, slot, ring, zr).wait_send()
            for kind in range(4):
                send2(col, kind, slot, ring, zr).start()

    def stage3(c, zr):
        slot, ring = c % DEP, c % RING
        h = zr // 2
        for col in range(2):
            fc, sc = axes[col][0][2], axes[col][1][2]
            for kind in range(2):
                send2(col, kind, slot, ring, zr).wait_recv()
                step, low = ((1, 0), (3, h))[kind]
                at = (ring, col, fc * 4 + (sc + step) % 4, pl.ds(low, h))
                part[at] = (f32(part[at]) + f32(r2[slot, col, kind, 0:h])).astype(BF)
                send2(col, 4 + kind, slot, ring, zr).start()
            for kind in range(4, 6):
                send1(col, kind, slot, ring, zr).wait_send()

    def stage4(c, zr, out, first):
        slot, ring = c % DEP, c % RING
        h = zr // 2
        for col in range(2):
            fc, sc = axes[col][0][2], axes[col][1][2]
            for kind in range(2, 6):
                send2(col, kind, slot, ring, zr).wait_recv()
            cols = pl.ds(pl.multiple_of((c - first) * 256 + col * 128, 128), 128)
            for half, (a, b) in enumerate(((4, 3), (2, 5))):
                own = part[ring, col, fc * 4 + sc, half * h : (half + 1) * h]
                out[half * h : (half + 1) * h, cols] = (
                    f32(own) + f32(r2[slot, col, a, 0:h]) + f32(r2[slot, col, b, 0:h])
                ).astype(BF)
            for kind in range(6):
                send2(col, kind, slot, ring, zr).wait_send()

    def both(c, fn, on_down, on_gate):
        @pl.when(jnp.logical_and(c >= 0, c < ND))
        def _():
            fn(c, *on_down)

        @pl.when(jnp.logical_and(c >= ND, c < NC))
        def _():
            fn(c, *on_gate)

    ZD, ZG = FF // 16, D // 16

    def down_rhs(c):
        return dy[:, pl.ds(pl.multiple_of(c * 256, 256), 256)]

    def gate_rhs(c):
        return pg[:, pl.ds(pl.multiple_of((c - ND) * 256, 256), 256)]

    def hidden_grad(f):
        a = pl.ds(pl.multiple_of(f * 256, 256), 256)
        b = pl.ds(pl.multiple_of(FF + f * 256, 256), 256)
        hg = nt(dy[...], dn[a, :])
        score = jnp.sum(f32(hid[:, a]) * hg, axis=1, keepdims=True)
        psum[...] = jnp.where(f == 0, 0.0, psum[...]) + score
        pg[:, a] = (f32(pg[:, a]) * hg).astype(BF)
        pg[:, b] = (f32(pg[:, b]) * hg).astype(BF)

    def ps_copy(q):
        return pltpu.make_async_remote_copy(
            src_ref=psend.at[q], dst_ref=precv.at[INV[q]], send_sem=ps_s.at[q], recv_sem=ps_r.at[INV[q]],
            device_id=(dp, place[q]), device_id_type=MESH,
        )

    def send_scores():
        for q in range(SRC):
            row = jnp.sum(pick(q) * psum[q * CAP : (q + 1) * CAP, :], axis=0, keepdims=True)
            if q == 0:
                precv[0] = jnp.broadcast_to(row, (8, TOK))
            else:
                psend[q] = jnp.broadcast_to(row, (8, TOK))
        for q in range(1, SRC):
            ps_copy(q).start()

    def row_grad(k):
        at = pl.ds(pl.multiple_of(k * 256, 256), 256)
        rg[:, at] = nt(pg[...], gu[at, :]).astype(BF)

    HALF = D // 2

    def rt_copy(q, half):
        cols = pl.ds(half * HALF, HALF)
        return pltpu.make_async_remote_copy(
            src_ref=rg.at[pl.ds(q * CAP, CAP), cols], dst_ref=rb.at[pl.ds(INV[q] * CAP, CAP), cols],
            send_sem=rt_s.at[half, q], recv_sem=rt_r.at[half, INV[q]],
            device_id=(dp, place[q]), device_id_type=MESH,
        )

    def rt_wait(q, half):
        cols = pl.ds(half * HALF, HALF)
        pltpu.make_async_remote_copy(
            src_ref=rg.at[pl.ds(q * CAP, CAP), cols], dst_ref=rb.at[pl.ds(q * CAP, CAP), cols],
            send_sem=rt_s.at[half, q], recv_sem=rt_r.at[half, q],
            device_id=(dp, place[q]), device_id_type=MESH,
        ).wait_recv()

    def send_rows(half):
        for q in range(1, SRC):
            rt_copy(q, half).start()
        cols = slice(half * HALF, (half + 1) * HALF)
        rb[0:CAP, cols] = rg[0:CAP, cols]

    def logit_grad():
        for q in range(1, SRC):
            pltpu.make_async_remote_copy(
                src_ref=psend.at[q], dst_ref=precv.at[q], send_sem=ps_s.at[q], recv_sem=ps_r.at[q],
                device_id=(dp, place[q]), device_id_type=MESH,
            ).wait_recv()
        for q in range(1, SRC):
            ps_copy(q).wait_send()
        scores = jnp.zeros((ROUTED, TOK), F32)
        for q in range(SRC):
            scores = jnp.where(sub == place[q], precv[q, 0:1, :], scores)
        scores = scores.T
        mean = jnp.sum(scores, axis=1, keepdims=True)
        z = jnp.sum(jnp.where(sub == lane, z_ref[...], 0.0), axis=1, keepdims=True)
        lgt = logit[...]
        log_total = jnp.log(jnp.sum(jnp.exp(lgt), axis=1, keepdims=True))
        z_grad = 2.0 * z * log_total * jnp.exp(lgt - log_total)
        lgrad[...] = (z_grad + scores - prob[...] * mean).astype(BF)

    def gate_copy(k):
        cols = pl.ds(pl.multiple_of(k * 256, 256), 256)
        return pltpu.make_async_copy(gug_out.at[:, cols], gug_hbm.at[:, cols], osem.at[k])

    def out_copy(k):
        a, b = ((dng_out, dng_hbm), (tg_out, tg_hbm), (rt_out, rt_hbm))[k]
        return pltpu.make_async_copy(a, b, osem.at[NG + k])

    def token_grad(half):
        for q in range(1, SRC):
            rt_wait(q, half)
        for q in range(1, SRC):
            rt_copy(q, half).wait_send()
        if half == 0:
            for q in range(SRC):
                sel[q * CAP : (q + 1) * CAP, :] = (
                    slot_of == meta[0, pl.ds(8 + place[q], 1), :]
                ).astype(F32).astype(BF)
        chosen = sel[...]
        grad = lgrad[...]

        def one(k, _):
            at = pl.ds(pl.multiple_of(k * 256, 256), 256)
            tg_out[:, at] = (tn(chosen, rb[:, at]) + nt(grad, rw_ref[at, :])).astype(BF)
            return 0

        lax.fori_loop(half * 4, half * 4 + 4, one, 0)
        if half == 1:
            out_copy(1).start()

    def ra_copy(q):
        return pltpu.make_async_remote_copy(
            src_ref=rpart.at[place[q]], dst_ref=rin.at[INV[q]], send_sem=ra_s.at[q], recv_sem=ra_r.at[INV[q]],
            device_id=(dp, place[q]), device_id_type=MESH,
        )

    def ra_wait(q):
        pltpu.make_async_remote_copy(
            src_ref=rpart.at[place[q]], dst_ref=rin.at[q], send_sem=ra_s.at[q], recv_sem=ra_r.at[q],
            device_id=(dp, place[q]), device_id_type=MESH,
        ).wait_recv()

    c1, c2 = pz + pc * (px - pz), px + pc * (pz - px)

    def to1(k):
        return zs(k) + pc * (xs(k) - zs(k))

    def to2(k):
        return xs(k) + pc * (zs(k) - xs(k))

    def rsz(k):
        return pltpu.make_async_remote_copy(
            src_ref=rsum.at[:, (c1 + k) % 4], dst_ref=rbufz.at[k], send_sem=rs_s.at[0, k], recv_sem=rs_r.at[0, k],
            device_id=(to1(k), ex), device_id_type=MESH,
        )

    def rsx(k):
        return pltpu.make_async_remote_copy(
            src_ref=rsumx.at[(c2 + k) % 4], dst_ref=rbufx.at[k], send_sem=rs_s.at[1, k], recv_sem=rs_r.at[1, k],
            device_id=(to2(k), ex), device_id_type=MESH,
        )

    def rcx(k, at):
        block = rt_out.at[ex, at, c1]
        return pltpu.make_async_remote_copy(
            src_ref=block, dst_ref=block, send_sem=rs_s.at[2, k], recv_sem=rs_r.at[2, k],
            device_id=(to2(k), ex), device_id_type=MESH,
        )

    def rcz(k, at):
        block = rt_out.at[ex, :, at]
        return pltpu.make_async_remote_copy(
            src_ref=block, dst_ref=block, send_sem=rs_s.at[3, k], recv_sem=rs_r.at[3, k],
            device_id=(to1(k), ex), device_id_type=MESH,
        )

    SAME = (2, 4, 6)

    def rd_copy(q, to_q):
        block = rt_out.at[place[q]]
        return pltpu.make_async_remote_copy(
            src_ref=block, dst_ref=block, send_sem=rd_s.at[q, to_q],
            recv_sem=rd_r.at[INV[to_q] if to_q != 1 else q + 1],
            device_id=(dp, place[to_q]), device_id_type=MESH,
        )

    def rd_wait(q):
        block = rt_out.at[place[q]]
        pltpu.make_async_remote_copy(
            src_ref=block, dst_ref=block, send_sem=rd_s.at[0, 1], recv_sem=rd_r.at[q],
            device_id=(dp, place[1]), device_id_type=MESH,
        ).wait_recv()

    def router_a():
        grad = lgrad[...]

        def one(b, _):
            at = pl.ds(pl.multiple_of(b * 256, 256), 256)
            rpart[b] = tn(xa[0, :, at], grad).astype(BF)
            return 0

        lax.fori_loop(0, SRC, one, 0)
        for q in range(1, SRC):
            ra_copy(q).start()

    def router_b():
        for q in range(1, SRC):
            ra_wait(q)
        acc = f32(rpart[ex])
        for q in range(1, SRC):
            acc = acc + f32(rin[q])
        rsum[...] = acc.reshape(4, 4, 16, ROUTED).astype(BF)
        for k in range(1, 4):
            rsz(k).start()

    def router_c():
        acc = f32(rsum[:, c1])
        for k in range(1, 4):
            rsz(k).wait_recv()
            acc = acc + f32(rbufz[k])
        rsumx[...] = acc.astype(BF)
        for k in range(1, 4):
            rsx(k).start()

    def router_x():
        acc = f32(rsumx[c2])
        for k in range(1, 4):
            rsx(k).wait_recv()
            acc = acc + f32(rbufx[k])
        rt_out[ex, c2, c1] = acc
        for k in range(1, 4):
            rcx(k, c2).start()

    def router_z():
        for k in range(1, 4):
            rcx(k, (c2 + 4 - k) % 4).wait_recv()
        for k in range(1, 4):
            rcz(k, c1).start()

    def router_d():
        for k in range(1, 4):
            rcz(k, (c1 + 4 - k) % 4).wait_recv()
        for to_q in SAME:
            rd_copy(0, to_q).start()
        rd_copy(0, 1).start()

    def router_e():
        for q in SAME:
            rd_wait(q)
            rd_copy(q, 1).start()

    def router_end():
        for q in (1, 3, 5, 7):
            rd_wait(q)
        for q in range(1, SRC):
            ra_copy(q).wait_send()
        for to_q in SAME:
            rd_copy(0, to_q).wait_send()
        for q in (0,) + SAME:
            rd_copy(q, 1).wait_send()
        for k in range(1, 4):
            rsz(k).wait_send()
            rsx(k).wait_send()
            rcx(k, c2).wait_send()
            rcz(k, c1).wait_send()
        out_copy(2).start()

    def body(i, _):
        @pl.when(i < ND)
        def _():
            compute(i, hidt, down_rhs, ZD)

        @pl.when(jnp.logical_and(i >= ND, i < NC))
        def _():
            compute(i, xt, gate_rhs, ZG)

        def parts(k):
            if k == 0:
                ag_relay(3)
                ag_own(4)
                grad_part(2)
            elif k == 1:
                ag_near(3)
                grad_part(3)
                ag_relay(4)
                ag_own(5)
            elif k == 2:
                ag_near(4)
            elif k == 3:
                grad_part(4)
                ag_relay(5)
            elif k == 4:
                ag_near(5)
                grad_part(5)
            else:
                for n in range(6):
                    for c in ALL:
                        ag(n, c).wait_send()
                for c in meta_sent:
                    c.wait_send()

        for k in range(6):
            pl.when(i == k)(functools.partial(parts, k))

        @pl.when(jnp.logical_and(i >= 5, i < 8))
        def _():
            hidden_grad(2 * i - 10)
            hidden_grad(2 * i - 9)

        @pl.when(i < 8)
        def _():
            flip(i)

        @pl.when(i == 7)
        def _():
            send_scores()

        @pl.when(jnp.logical_and(i >= ND, i < ND + 4))
        def _():
            row_grad(2 * (i - ND))
            row_grad(2 * (i - ND) + 1)

        for at, step in (
            (ND, logit_grad), (ND, router_a), (ND + 4, router_b), (ND + 5, router_c),
            (ND + 6, router_x), (ND + 7, router_z), (ND + 8, router_d), (NC - 1, router_e), (NC + 1, router_end),
            (ND + 1, functools.partial(send_rows, 0)), (ND + 3, functools.partial(send_rows, 1)),
            (NC - 3, functools.partial(token_grad, 0)), (NC - 1, functools.partial(token_grad, 1)),
        ):
            pl.when(i == at)(step)

        c4 = i - LAG4

        @pl.when(jnp.logical_and(c4 >= 0, c4 < ND))
        def _():
            stage4(c4, ZD, dng_out, 0)

        @pl.when(c4 == ND - 1)
        def _():
            out_copy(0).start()

        @pl.when(c4 >= ND)
        def _():
            stage4(c4, ZG, gug_out, ND)
            gate_copy(c4 - ND).start()

        both(i - LAG3, stage3, (ZD,), (ZG,))
        both(i - LAG2, stage2, (ZD,), (ZG,))
        both(i - LAG1, stage1, (ZD,), (ZG,))
        return 0

    lax.fori_loop(0, NC + LAG4, body, 0)
    for k in range(NG):
        gate_copy(k).wait()
    for k in range(3):
        out_copy(k).wait()


def write_out(*refs):
    src, dst, held, sems = refs[0:4], refs[4:8], refs[8:12], refs[12]
    pieces = []
    for k in range(4):
        n = src[k].shape[0] // 2
        for half in range(2):
            at = pl.ds(half * n, n)
            pieces.append(
                (
                    pltpu.make_async_copy(src[k].at[at], held[k].at[at], sems.at[0, k, half]),
                    pltpu.make_async_copy(held[k].at[at], dst[k].at[at], sems.at[1, k, half]),
                )
            )
    for load, _ in pieces:
        load.start()
    for load, store in pieces:
        load.wait()
        store.start()
    for _, store in pieces:
        store.wait()


def per_device(tokens, out_grad, z_weight, router_weight, expert_ids, gate_up_weight, down_weight):
    hbm = pl.BlockSpec(memory_space=pl.ANY)
    dma = pltpu.SemaphoreType.DMA
    outs = pl.pallas_call(
        kernel,
        out_shape=(
            jax.ShapeDtypeStruct((TOK, D), BF),
            jax.ShapeDtypeStruct((SRC, 4, 4, 16, ROUTED), F32),
            jax.ShapeDtypeStruct((D // 16, 2 * FF), BF),
            jax.ShapeDtypeStruct((FF // 16, D), BF),
        ),
        in_specs=[hbm] * 7,
        out_specs=(hbm, hbm, hbm, hbm),
        scratch_shapes=[
            pltpu.VMEM((1, TOK), F32),
            pltpu.VMEM((D, ROUTED), BF),
            pltpu.VMEM((4, TOK), jnp.int32),
            pltpu.VMEM((TOK, D), BF),
            pltpu.VMEM((SRC, 4, 4, 16, ROUTED), F32),
            pltpu.VMEM((D // 16, 2 * FF), BF),
            pltpu.VMEM((FF // 16, D), BF),
            pltpu.VMEM((SRC, TOK, D), BF),
            pltpu.VMEM((SRC, TOK, D), BF),
            pltpu.VMEM((SRC, 16, TOK), F32),
            pltpu.VMEM((TOK, ROUTED), F32),
            pltpu.VMEM((TOK, ROUTED), F32),
            pltpu.VMEM((ROWS, D), BF),
            pltpu.VMEM((D, ROWS), BF),
            pltpu.VMEM((ROWS, D), BF),
            pltpu.VMEM((ROWS, FF), BF),
            pltpu.VMEM((FF, ROWS), BF),
            pltpu.VMEM((ROWS, 2 * FF), BF),
            pltpu.VMEM((D, 2 * FF), BF),
            pltpu.VMEM((FF, D), BF),
            pltpu.VMEM((RING, 2, 16, 128, 128), BF),
            pltpu.VMEM((DEP, 2, 6, 2, 128, 128), BF),
            pltpu.VMEM((DEP, 2, 6, 64, 128), BF),
            pltpu.VMEM((ROWS, D), BF),
            pltpu.VMEM((ROWS, D), BF),
            pltpu.VMEM((ROWS, TOK), BF),
            pltpu.VMEM((ROWS, 1), F32),
            pltpu.VMEM((SRC, 8, TOK), F32),
            pltpu.VMEM((SRC, 8, TOK), F32),
            pltpu.VMEM((TOK, ROUTED), BF),
            pltpu.VMEM((SRC, D // SRC, ROUTED), BF),
            pltpu.VMEM((SRC, D // SRC, ROUTED), BF),
            pltpu.VMEM((4, 4, 16, ROUTED), BF),
            pltpu.VMEM((4, 4, 16, ROUTED), BF),
            pltpu.VMEM((4, 16, ROUTED), BF),
            pltpu.VMEM((4, 16, ROUTED), BF),
            dma((7,)), dma((NG + 3,)),
            dma((6, 14)), dma((6, SRC, 2)),
            dma((SRC,)), dma((SRC,)),
            dma((SRC,)), dma((SRC,)),
            dma((2, SRC)), dma((2, SRC)),
            dma((DEP, 2, 6)), dma((DEP, 2, 6)),
            dma((DEP, 2, 6)), dma((DEP, 2, 6)),
            dma((SRC,)), dma((SRC,)),
            dma((4, 4)), dma((4, 4)),
            dma((SRC, SRC)), dma((SRC,)),
        ],
        compiler_params=pltpu.CompilerParams(
            collective_id=0, has_side_effects=True, vmem_limit_bytes=67043328
        ),
        name="moe_backward",
    )(
        tokens, out_grad, z_weight.reshape(1, TOK), router_weight, expert_ids.T,
        gate_up_weight[0], down_weight[0],
    )
    shapes = tuple(jax.ShapeDtypeStruct(o.shape, o.dtype) for o in outs)
    token_grad, router_grad, gate_up_grad, down_grad = pl.pallas_call(
        write_out,
        out_shape=shapes,
        in_specs=[hbm] * 4,
        out_specs=[hbm] * 4,
        scratch_shapes=[pltpu.VMEM(o.shape, o.dtype) for o in shapes] + [dma((2, 4, 2))],
        name="write_out",
    )(*outs)
    return token_grad, router_grad.reshape(D, ROUTED), gate_up_grad[None], down_grad[None]


def solution(mesh):
    return jax.shard_map(
        per_device,
        mesh=mesh,
        in_specs=(
            P(("dp", "expert"), None),
            P(("dp", "expert"), None),
            P(("dp", "expert")),
            P(),
            P(("dp", "expert"), None),
            P("expert", None, None),
            P("expert", None, None),
        ),
        out_specs=(
            P(("dp", "expert"), None),
            P(),
            P("expert", "dp", None),
            P("expert", "dp", None),
        ),
        check_vma=False,
    )
```

```python
import functools

import jax
import jax.numpy as jnp
from jax import lax
from jax.experimental import pallas as pl
from jax.experimental.pallas import tpu as pltpu
from jax.sharding import PartitionSpec as P

BF = jnp.bfloat16
F32 = jnp.float32
MESH = pl.DeviceIdType.MESH

TOK = 128
CAP = 64
D = 2048
FF = 1536
SRC = 8
NDP = 16
ROWS = SRC * CAP
ROUTED = 128
ND = D // 256
NG = 2 * FF // 256
NC = ND + NG
LAG1, LAG2, LAG3, LAG4 = 1, 3, 4, 6
DEP = 6
RING = 7
CUTS = (0, 256, 512, 1024, 1536, 2048)
INV = (0, 1, 4, 5, 2, 3, 6, 7)


def nt(a, b):
    return lax.dot_general(a, b, (((1,), (1,)), ((), ())), preferred_element_type=F32)


def tn(a, b):
    return lax.dot_general(a, b, (((0,), (0,)), ((), ())), preferred_element_type=F32)


def nn(a, b):
    return jnp.dot(a, b, preferred_element_type=F32)


def kernel(
    tokens_hbm, grad_hbm, z_hbm, rw_hbm, ids_hbm, gu_hbm, dn_hbm,
    tg_hbm, rt_hbm, gug_hbm, dng_hbm,
    z_ref, rw_ref, ids_ref, tg_out, rt_out, gug_out, dng_out,
    xa, oa, meta, prob, logit, xr, xt, dy, hid, hidt, pg, gu, dn,
    part, r1, r2, rg, rb, sel, psum, psend, precv, lgrad, rpart, rin, rsum, rbufz, rsumx, rbufx,
    lsem, osem, ag_s, ag_r, mt_s, mt_r, ps_s, ps_r, rt_s, rt_r, s1, q1, s2, q2, ra_s, ra_r, rs_s, rs_r, rd_s, rd_r,
):
    dp = lax.axis_index("dp")
    ex = lax.axis_index("expert")
    px, pz = dp // 4, dp % 4
    py, pc = ex // 2, ex % 2

    def xs(k):
        return ((px + k) % 4) * 4 + pz

    def zs(k):
        return px * 4 + (pz + k) % 4

    xp, xm, zp, zm = xs(1), xs(3), zs(1), zs(3)
    yp, ym, yo = (py + 1) % 4, (py + 3) % 4, (py + 2) % 4
    oc = 1 - pc
    place = (ex, py * 2 + oc, ym * 2 + pc, ym * 2 + oc, yp * 2 + pc, yp * 2 + oc, yo * 2 + pc, yo * 2 + oc)

    cp_tok = pltpu.make_async_copy(tokens_hbm, xa.at[0], lsem.at[0])
    cp_grad = pltpu.make_async_copy(grad_hbm, oa.at[0], lsem.at[1])
    cp_gu = pltpu.make_async_copy(gu_hbm, gu, lsem.at[2])
    cp_dn = pltpu.make_async_copy(dn_hbm, dn, lsem.at[3])
    cp_rw = pltpu.make_async_copy(rw_hbm, rw_ref, lsem.at[4])
    cp_z = pltpu.make_async_copy(z_hbm, z_ref, lsem.at[5])
    cp_ids = pltpu.make_async_copy(ids_hbm, ids_ref, lsem.at[6])
    cp_tok.start()

    barrier = pltpu.get_barrier_semaphore()
    for k in range(1, 4):
        pl.semaphore_signal(barrier, inc=1, device_id=(xs(k), ex), device_id_type=MESH)
        pl.semaphore_signal(barrier, inc=1, device_id=(zs(k), ex), device_id_type=MESH)
    for q in range(1, SRC):
        pl.semaphore_signal(barrier, inc=1, device_id=(dp, place[q]), device_id_type=MESH)
    cp_rw.start()
    cp_ids.start()
    cp_z.start()
    cp_grad.start()
    cp_gu.start()
    cp_dn.start()
    pl.semaphore_wait(barrier, 6 + SRC - 1)

    OWN = ((0, 0, 4, 2), (0, 1, 2, 4), (0, 1, 4, 2), (0, 0, 2, 4), (0, 0, 1, 1), (0, 1, 1, 1))
    RELAY = ((2, 0, 4, 6), (2, 0, 1, 3), (4, 1, 2, 6), (4, 1, 1, 5))
    NEAR = ((2, 1, 1, 3), (4, 0, 1, 5))
    FAR = ((6, 0, 1, 7), (6, 1, 1, 7))
    ALL = OWN + RELAY + NEAR + FAR

    def ag_view(part_no, q, half):
        rows = pl.ds(half * CAP, CAP)
        if part_no == 0:
            return xa.at[q, rows]
        return oa.at[q, rows, pl.ds(CUTS[part_no - 1], CUTS[part_no] - CUTS[part_no - 1])]

    def ag(part_no, copy):
        src_q, half, to_q, dst_q = copy
        return pltpu.make_async_remote_copy(
            src_ref=ag_view(part_no, src_q, half), dst_ref=ag_view(part_no, dst_q, half),
            send_sem=ag_s.at[part_no, ALL.index(copy)], recv_sem=ag_r.at[part_no, dst_q, half],
            device_id=(dp, place[to_q]), device_id_type=MESH,
        )

    def ag_wait(part_no, q, half):
        pltpu.make_async_remote_copy(
            src_ref=ag_view(part_no, q, half), dst_ref=ag_view(part_no, q, half),
            send_sem=ag_s.at[part_no, 0], recv_sem=ag_r.at[part_no, q, half],
            device_id=(dp, place[1]), device_id_type=MESH,
        ).wait_recv()

    def ag_own(part_no):
        for c in OWN:
            ag(part_no, c).start()

    def ag_relay(part_no):
        ag_wait(part_no, 2, 0)
        ag(part_no, RELAY[0]).start()
        ag(part_no, RELAY[1]).start()
        ag_wait(part_no, 4, 1)
        ag(part_no, RELAY[2]).start()
        ag(part_no, RELAY[3]).start()

    def ag_near(part_no):
        ag_wait(part_no, 2, 1)
        ag(part_no, NEAR[0]).start()
        ag_wait(part_no, 4, 0)
        ag(part_no, NEAR[1]).start()

    def ag_far(part_no):
        for half in range(2):
            ag_wait(part_no, 6, half)
            ag(part_no, FAR[half]).start()

    def ag_side(part_no, q):
        ag_wait(part_no, q, 0)
        ag_wait(part_no, q, 1)

    cp_tok.wait()
    ag_own(0)

    sub = lax.broadcasted_iota(jnp.int32, (TOK, TOK), 0)
    lane = lax.broadcasted_iota(jnp.int32, (TOK, TOK), 1)
    cp_rw.wait()
    cp_ids.wait()
    cp_z.wait()
    lg = nn(xa[0], rw_ref[...])
    logit[...] = lg
    ids = ids_ref[...].astype(F32)
    ids = jnp.concatenate([ids, ids], axis=0).T
    lane_f = lane.astype(F32)
    dense = jnp.zeros((TOK, ROUTED), F32)
    mask = jnp.zeros((TOK, ROUTED), F32)
    total = jnp.zeros((TOK, 1), F32)
    for k in range(4):
        hit = ids[:, k : k + 1] == lane_f
        value = jnp.exp(jnp.sum(jnp.where(hit, lg, 0.0), axis=1, keepdims=True))
        total = total + value
        dense = jnp.where(hit, value, dense)
        mask = jnp.where(hit, 1.0, mask)
    dense = dense / total
    prob[...] = dense
    before = jnp.where(lane < sub, 1.0, 0.0).astype(BF)
    rank = nn(before, mask.astype(BF))
    rank = jnp.where(mask > 0.5, rank, -1.0)
    meta[0, 0:8, :] = dense.T[0:8]
    meta[0, 8:16, :] = rank.T[0:8]
    meta_sent = []
    for q in range(1, SRC):
        c = pltpu.make_async_remote_copy(
            src_ref=meta.at[0], dst_ref=meta.at[INV[q]], send_sem=mt_s.at[q], recv_sem=mt_r.at[INV[q]],
            device_id=(dp, place[q]), device_id_type=MESH,
        )
        c.start()
        meta_sent.append(c)

    cp_grad.wait()
    ag_own(1)
    ag_relay(0)
    ag_own(2)
    ag_near(0)

    for q in range(1, SRC):
        pltpu.make_async_remote_copy(
            src_ref=meta.at[0], dst_ref=meta.at[q], send_sem=mt_s.at[q], recv_sem=mt_r.at[q],
            device_id=(dp, place[q]), device_id_type=MESH,
        ).wait_recv()

    slot_of = lax.broadcasted_iota(jnp.int32, (CAP, TOK), 0).astype(F32)

    def pick(q):
        return (slot_of == meta[q, pl.ds(8 + ex, 1), :]).astype(F32)

    def gather_tok(q):
        rows = nn(pick(q).astype(BF), xa[q]).astype(BF)
        xr[q * CAP : (q + 1) * CAP, :] = rows

    def gather_grad(q, part_no):
        p = pick(q)
        weight = jnp.sum(p * meta[q, pl.ds(ex, 1), :], axis=1, keepdims=True)
        cols = slice(CUTS[part_no - 1], CUTS[part_no])
        rows = nn(p.astype(BF), oa[q, :, cols])
        dy[q * CAP : (q + 1) * CAP, cols] = (weight * rows).astype(BF)

    def grad_near(part_no):
        for q in (1, 3, 5):
            ag_side(part_no, q)
        for q in range(6):
            gather_grad(q, part_no)

    def grad_far(part_no):
        ag_far(part_no)
        gather_grad(6, part_no)
        ag_side(part_no, 7)
        gather_grad(7, part_no)

    def grad_part(part_no):
        grad_near(part_no)
        grad_far(part_no)

    def forward(lo, hi, n):
        def run(f, _):
            a = pl.ds(pl.multiple_of(f * n, n), n)
            b = pl.ds(pl.multiple_of(FF + f * n, n), n)
            g = nn(xr[lo:hi, :], gu[:, a])
            u = nn(xr[lo:hi, :], gu[:, b])
            s = lax.logistic(g)
            act = g * s
            h = (act * u).astype(BF)
            hid[lo:hi, a] = h
            hidt[a, lo:hi] = h.T
            pg[lo:hi, a] = (u * s * (1.0 + g * (1.0 - s))).astype(BF)
            pg[lo:hi, b] = act.astype(BF)
            return 0

        return run

    near, far = forward(0, 6 * CAP, 256), forward(6 * CAP, ROWS, 512)
    for q in (1, 3, 5):
        ag_side(0, q)
    for q in range(6):
        gather_tok(q)
    cp_gu.wait()
    lax.fori_loop(0, 6, near, 0)
    ag_relay(1)
    ag_own(3)
    ag_far(0)
    gather_tok(6)
    ag_near(1)
    ag_side(0, 7)
    gather_tok(7)
    lax.fori_loop(0, 2, far, 0)
    ag_relay(2)
    lax.fori_loop(2, 3, far, 0)
    ag_near(2)
    grad_part(1)
    cp_dn.wait()

    def flip(k):
        a = pl.ds(pl.multiple_of(k * 256, 256), 256)
        xt[a, :] = xr[:, a].T

    axes = (((xp, xm, px), (zp, zm, pz)), ((zp, zm, pz), (xp, xm, px)))

    def send1(col, kind, slot, ring, zr):
        plus, minus, fc = axes[col][0]
        base = (
            ((fc + 2) % 4) * 4, ((fc + 2) % 4) * 4 + 2,
            ((fc + 1) % 4) * 4 + 2, ((fc + 3) % 4) * 4,
            ((fc + 1) % 4) * 4, ((fc + 3) % 4) * 4 + 2,
        )[kind]
        return pltpu.make_async_remote_copy(
            src_ref=part.at[ring, col, pl.ds(base, 2), pl.ds(0, zr)],
            dst_ref=r1.at[slot, col, kind, :, pl.ds(0, zr)],
            send_sem=s1.at[slot, col, kind], recv_sem=q1.at[slot, col, kind],
            device_id=(plus if kind % 2 == 0 else minus, ex), device_id_type=MESH,
        )

    def send2(col, kind, slot, ring, zr):
        plus, minus, sc = axes[col][1]
        fc = axes[col][0][2]
        h = zr // 2
        step, low = ((2, 0), (2, h), (1, h), (3, 0), (1, 0), (3, h))[kind]
        return pltpu.make_async_remote_copy(
            src_ref=part.at[ring, col, fc * 4 + (sc + step) % 4, pl.ds(low, h)],
            dst_ref=r2.at[slot, col, kind, pl.ds(0, h)],
            send_sem=s2.at[slot, col, kind], recv_sem=q2.at[slot, col, kind],
            device_id=(plus if kind % 2 == 0 else minus, ex), device_id_type=MESH,
        )

    def f32(v):
        return v.astype(F32)

    def compute(c, lhs, rhs_of, zr):
        slot, ring = c % DEP, c % RING
        rhs = rhs_of(c)
        rows = 4 * zr

        def one(b, _):
            r = nn(lhs[pl.ds(pl.multiple_of(b * rows, rows), rows), :], rhs).astype(BF)
            for k in range(4):
                part[ring, 0, b * 4 + k, 0:zr] = r[k * zr : (k + 1) * zr, 0:128]
                part[ring, 1, k * 4 + b, 0:zr] = r[k * zr : (k + 1) * zr, 128:256]
            return 0

        lax.fori_loop(0, 4, one, 0)
        for kind in range(4):
            for col in range(2):
                send1(col, kind, slot, ring, zr).start()

    def stage1(c, zr):
        slot, ring = c % DEP, c % RING
        for col in range(2):
            fc = axes[col][0][2]
            for kind in range(2):
                send1(col, kind, slot, ring, zr).wait_recv()
                base = ((fc + 1) % 4) * 4 if kind == 0 else ((fc + 3) % 4) * 4 + 2
                at = (ring, col, pl.ds(base, 2), pl.ds(0, zr))
                part[at] = (f32(part[at]) + f32(r1[slot, col, kind, :, 0:zr])).astype(BF)
                send1(col, 4 + kind, slot, ring, zr).start()

    def stage2(c, zr):
        slot, ring = c % DEP, c % RING
        for col in range(2):
            fc = axes[col][0][2]
            for kind in range(2, 6):
                send1(col, kind, slot, ring, zr).wait_recv()
            for half, (a, b) in enumerate(((4, 3), (2, 5))):
                at = (ring, col, pl.ds(fc * 4 + 2 * half, 2), pl.ds(0, zr))
                part[at] = (
                    f32(part[at]) + f32(r1[slot, col, a, :, 0:zr]) + f32(r1[slot, col, b, :, 0:zr])
                ).astype(BF)
            for kind in range(4):
                send1(col, kind, slot, ring, zr).wait_send()
            for kind in range(4):
                send2(col, kind, slot, ring, zr).start()

    def stage3(c, zr):
        slot, ring = c % DEP, c % RING
        h = zr // 2
        for col in range(2):
            fc, sc = axes[col][0][2], axes[col][1][2]
            for kind in range(2):
                send2(col, kind, slot, ring, zr).wait_recv()
                step, low = ((1, 0), (3, h))[kind]
                at = (ring, col, fc * 4 + (sc + step) % 4, pl.ds(low, h))
                part[at] = (f32(part[at]) + f32(r2[slot, col, kind, 0:h])).astype(BF)
                send2(col, 4 + kind, slot, ring, zr).start()
            for kind in range(4, 6):
                send1(col, kind, slot, ring, zr).wait_send()

    def stage4(c, zr, out, first):
        slot, ring = c % DEP, c % RING
        h = zr // 2
        for col in range(2):
            fc, sc = axes[col][0][2], axes[col][1][2]
            for kind in range(2, 6):
                send2(col, kind, slot, ring, zr).wait_recv()
            cols = pl.ds(pl.multiple_of((c - first) * 256 + col * 128, 128), 128)
            for half, (a, b) in enumerate(((4, 3), (2, 5))):
                own = part[ring, col, fc * 4 + sc, half * h : (half + 1) * h]
                out[half * h : (half + 1) * h, cols] = (
                    f32(own) + f32(r2[slot, col, a, 0:h]) + f32(r2[slot, col, b, 0:h])
                ).astype(BF)
            for kind in range(6):
                send2(col, kind, slot, ring, zr).wait_send()

    def both(c, fn, on_down, on_gate):
        @pl.when(jnp.logical_and(c >= 0, c < ND))
        def _():
            fn(c, *on_down)

        @pl.when(jnp.logical_and(c >= ND, c < NC))
        def _():
            fn(c, *on_gate)

    ZD, ZG = FF // 16, D // 16

    def down_rhs(c):
        return dy[:, pl.ds(pl.multiple_of(c * 256, 256), 256)]

    def gate_rhs(c):
        return pg[:, pl.ds(pl.multiple_of((c - ND) * 256, 256), 256)]

    def hidden_grad(f):
        a = pl.ds(pl.multiple_of(f * 256, 256), 256)
        b = pl.ds(pl.multiple_of(FF + f * 256, 256), 256)
        hg = nt(dy[...], dn[a, :])
        score = jnp.sum(f32(hid[:, a]) * hg, axis=1, keepdims=True)
        psum[...] = jnp.where(f == 0, 0.0, psum[...]) + score
        pg[:, a] = (f32(pg[:, a]) * hg).astype(BF)
        pg[:, b] = (f32(pg[:, b]) * hg).astype(BF)

    def ps_copy(q):
        return pltpu.make_async_remote_copy(
            src_ref=psend.at[q], dst_ref=precv.at[INV[q]], send_sem=ps_s.at[q], recv_sem=ps_r.at[INV[q]],
            device_id=(dp, place[q]), device_id_type=MESH,
        )

    def send_scores():
        for q in range(SRC):
            row = jnp.sum(pick(q) * psum[q * CAP : (q + 1) * CAP, :], axis=0, keepdims=True)
            if q == 0:
                precv[0] = jnp.broadcast_to(row, (8, TOK))
            else:
                psend[q] = jnp.broadcast_to(row, (8, TOK))
        for q in range(1, SRC):
            ps_copy(q).start()

    def row_grad(k):
        at = pl.ds(pl.multiple_of(k * 256, 256), 256)
        rg[:, at] = nt(pg[...], gu[at, :]).astype(BF)

    HALF = D // 2

    def rt_copy(q, half):
        cols = pl.ds(half * HALF, HALF)
        return pltpu.make_async_remote_copy(
            src_ref=rg.at[pl.ds(q * CAP, CAP), cols], dst_ref=rb.at[pl.ds(INV[q] * CAP, CAP), cols],
            send_sem=rt_s.at[half, q], recv_sem=rt_r.at[half, INV[q]],
            device_id=(dp, place[q]), device_id_type=MESH,
        )

    def rt_wait(q, half):
        cols = pl.ds(half * HALF, HALF)
        pltpu.make_async_remote_copy(
            src_ref=rg.at[pl.ds(q * CAP, CAP), cols], dst_ref=rb.at[pl.ds(q * CAP, CAP), cols],
            send_sem=rt_s.at[half, q], recv_sem=rt_r.at[half, q],
            device_id=(dp, place[q]), device_id_type=MESH,
        ).wait_recv()

    def send_rows(half):
        for q in range(1, SRC):
            rt_copy(q, half).start()
        cols = slice(half * HALF, (half + 1) * HALF)
        rb[0:CAP, cols] = rg[0:CAP, cols]

    def logit_grad():
        for q in range(1, SRC):
            pltpu.make_async_remote_copy(
                src_ref=psend.at[q], dst_ref=precv.at[q], send_sem=ps_s.at[q], recv_sem=ps_r.at[q],
                device_id=(dp, place[q]), device_id_type=MESH,
            ).wait_recv()
        for q in range(1, SRC):
            ps_copy(q).wait_send()
        scores = jnp.zeros((ROUTED, TOK), F32)
        for q in range(SRC):
            scores = jnp.where(sub == place[q], precv[q, 0:1, :], scores)
        scores = scores.T
        mean = jnp.sum(scores, axis=1, keepdims=True)
        z = jnp.sum(jnp.where(sub == lane, z_ref[...], 0.0), axis=1, keepdims=True)
        lgt = logit[...]
        log_total = jnp.log(jnp.sum(jnp.exp(lgt), axis=1, keepdims=True))
        z_grad = 2.0 * z * log_total * jnp.exp(lgt - log_total)
        lgrad[...] = (z_grad + scores - prob[...] * mean).astype(BF)

    def gate_copy(k):
        cols = pl.ds(pl.multiple_of(k * 256, 256), 256)
        return pltpu.make_async_copy(gug_out.at[:, cols], gug_hbm.at[:, cols], osem.at[k])

    def out_copy(k):
        a, b = ((dng_out, dng_hbm), (tg_out, tg_hbm), (rt_out, rt_hbm))[k]
        return pltpu.make_async_copy(a, b, osem.at[NG + k])

    def token_grad(half):
        for q in range(1, SRC):
            rt_wait(q, half)
        for q in range(1, SRC):
            rt_copy(q, half).wait_send()
        if half == 0:
            for q in range(SRC):
                sel[q * CAP : (q + 1) * CAP, :] = (
                    slot_of == meta[0, pl.ds(8 + place[q], 1), :]
                ).astype(F32).astype(BF)
        chosen = sel[...]
        grad = lgrad[...]

        def one(k, _):
            at = pl.ds(pl.multiple_of(k * 256, 256), 256)
            tg_out[:, at] = (tn(chosen, rb[:, at]) + nt(grad, rw_ref[at, :])).astype(BF)
            return 0

        lax.fori_loop(half * 4, half * 4 + 4, one, 0)
        if half == 1:
            out_copy(1).start()

    def ra_copy(q):
        return pltpu.make_async_remote_copy(
            src_ref=rpart.at[place[q]], dst_ref=rin.at[INV[q]], send_sem=ra_s.at[q], recv_sem=ra_r.at[INV[q]],
            device_id=(dp, place[q]), device_id_type=MESH,
        )

    def ra_wait(q):
        pltpu.make_async_remote_copy(
            src_ref=rpart.at[place[q]], dst_ref=rin.at[q], send_sem=ra_s.at[q], recv_sem=ra_r.at[q],
            device_id=(dp, place[q]), device_id_type=MESH,
        ).wait_recv()

    c1, c2 = pz + pc * (px - pz), px + pc * (pz - px)

    def to1(k):
        return zs(k) + pc * (xs(k) - zs(k))

    def to2(k):
        return xs(k) + pc * (zs(k) - xs(k))

    def rsz(k):
        return pltpu.make_async_remote_copy(
            src_ref=rsum.at[:, (c1 + k) % 4], dst_ref=rbufz.at[k], send_sem=rs_s.at[0, k], recv_sem=rs_r.at[0, k],
            device_id=(to1(k), ex), device_id_type=MESH,
        )

    def rsx(k):
        return pltpu.make_async_remote_copy(
            src_ref=rsumx.at[(c2 + k) % 4], dst_ref=rbufx.at[k], send_sem=rs_s.at[1, k], recv_sem=rs_r.at[1, k],
            device_id=(to2(k), ex), device_id_type=MESH,
        )

    def rcx(k, at):
        block = rt_out.at[ex, at, c1]
        return pltpu.make_async_remote_copy(
            src_ref=block, dst_ref=block, send_sem=rs_s.at[2, k], recv_sem=rs_r.at[2, k],
            device_id=(to2(k), ex), device_id_type=MESH,
        )

    def rcz(k, at):
        block = rt_out.at[ex, :, at]
        return pltpu.make_async_remote_copy(
            src_ref=block, dst_ref=block, send_sem=rs_s.at[3, k], recv_sem=rs_r.at[3, k],
            device_id=(to1(k), ex), device_id_type=MESH,
        )

    SAME = (2, 4, 6)

    def rd_copy(q, to_q):
        block = rt_out.at[place[q]]
        return pltpu.make_async_remote_copy(
            src_ref=block, dst_ref=block, send_sem=rd_s.at[q, to_q],
            recv_sem=rd_r.at[INV[to_q] if to_q != 1 else q + 1],
            device_id=(dp, place[to_q]), device_id_type=MESH,
        )

    def rd_wait(q):
        block = rt_out.at[place[q]]
        pltpu.make_async_remote_copy(
            src_ref=block, dst_ref=block, send_sem=rd_s.at[0, 1], recv_sem=rd_r.at[q],
            device_id=(dp, place[1]), device_id_type=MESH,
        ).wait_recv()

    def router_a():
        grad = lgrad[...]

        def one(b, _):
            at = pl.ds(pl.multiple_of(b * 256, 256), 256)
            rpart[b] = tn(xa[0, :, at], grad).astype(BF)
            return 0

        lax.fori_loop(0, SRC, one, 0)
        for q in range(1, SRC):
            ra_copy(q).start()

    def router_b():
        for q in range(1, SRC):
            ra_wait(q)
        acc = f32(rpart[ex])
        for q in range(1, SRC):
            acc = acc + f32(rin[q])
        rsum[...] = acc.reshape(4, 4, 16, ROUTED).astype(BF)
        for k in range(1, 4):
            rsz(k).start()

    def router_c():
        acc = f32(rsum[:, c1])
        for k in range(1, 4):
            rsz(k).wait_recv()
            acc = acc + f32(rbufz[k])
        rsumx[...] = acc.astype(BF)
        for k in range(1, 4):
            rsx(k).start()

    def router_x():
        acc = f32(rsumx[c2])
        for k in range(1, 4):
            rsx(k).wait_recv()
            acc = acc + f32(rbufx[k])
        rt_out[ex, c2, c1] = acc
        for k in range(1, 4):
            rcx(k, c2).start()

    def router_z():
        for k in range(1, 4):
            rcx(k, (c2 + 4 - k) % 4).wait_recv()
        for k in range(1, 4):
            rcz(k, c1).start()

    def router_d():
        for k in range(1, 4):
            rcz(k, (c1 + 4 - k) % 4).wait_recv()
        for to_q in SAME:
            rd_copy(0, to_q).start()
        rd_copy(0, 1).start()

    def router_e():
        for q in SAME:
            rd_wait(q)
            rd_copy(q, 1).start()

    def router_end():
        for q in (1, 3, 5, 7):
            rd_wait(q)
        for q in range(1, SRC):
            ra_copy(q).wait_send()
        for to_q in SAME:
            rd_copy(0, to_q).wait_send()
        for q in (0,) + SAME:
            rd_copy(q, 1).wait_send()
        for k in range(1, 4):
            rsz(k).wait_send()
            rsx(k).wait_send()
            rcx(k, c2).wait_send()
            rcz(k, c1).wait_send()
        out_copy(2).start()

    def body(i, _):
        @pl.when(i < ND)
        def _():
            compute(i, hidt, down_rhs, ZD)

        @pl.when(jnp.logical_and(i >= ND, i < NC))
        def _():
            compute(i, xt, gate_rhs, ZG)

        def parts(k):
            if k == 0:
                ag_relay(3)
                ag_own(4)
                grad_part(2)
            elif k == 1:
                ag_near(3)
                grad_part(3)
                ag_relay(4)
                ag_own(5)
            elif k == 2:
                ag_near(4)
            elif k == 3:
                grad_part(4)
                ag_relay(5)
            elif k == 4:
                ag_near(5)
                grad_part(5)
            else:
                for n in range(6):
                    for c in ALL:
                        ag(n, c).wait_send()
                for c in meta_sent:
                    c.wait_send()

        for k in range(6):
            pl.when(i == k)(functools.partial(parts, k))

        @pl.when(jnp.logical_and(i >= 5, i < 8))
        def _():
            hidden_grad(2 * i - 10)
            hidden_grad(2 * i - 9)

        @pl.when(i < 8)
        def _():
            flip(i)

        @pl.when(i == 7)
        def _():
            send_scores()

        @pl.when(jnp.logical_and(i >= ND, i < ND + 4))
        def _():
            row_grad(2 * (i - ND))
            row_grad(2 * (i - ND) + 1)

        for at, step in (
            (ND, logit_grad), (ND, router_a), (ND + 4, router_b), (ND + 5, router_c),
            (ND + 6, router_x), (ND + 7, router_z), (ND + 8, router_d), (NC - 1, router_e), (NC + 1, router_end),
            (ND + 1, functools.partial(send_rows, 0)), (ND + 3, functools.partial(send_rows, 1)),
            (NC - 3, functools.partial(token_grad, 0)), (NC - 1, functools.partial(token_grad, 1)),
        ):
            pl.when(i == at)(step)

        c4 = i - LAG4

        @pl.when(jnp.logical_and(c4 >= 0, c4 < ND))
        def _():
            stage4(c4, ZD, dng_out, 0)

        @pl.when(c4 == ND - 1)
        def _():
            out_copy(0).start()

        @pl.when(c4 >= ND)
        def _():
            stage4(c4, ZG, gug_out, ND)
            gate_copy(c4 - ND).start()

        both(i - LAG3, stage3, (ZD,), (ZG,))
        both(i - LAG2, stage2, (ZD,), (ZG,))
        both(i - LAG1, stage1, (ZD,), (ZG,))
        return 0

    lax.fori_loop(0, NC + LAG4, body, 0)
    for k in range(NG):
        gate_copy(k).wait()
    for k in range(3):
        out_copy(k).wait()


def write_out(*refs):
    src, dst, held, sems = refs[0:4], refs[4:8], refs[8:12], refs[12]
    pieces = []
    for k in range(4):
        n = src[k].shape[0] // 2
        for half in range(2):
            at = pl.ds(half * n, n)
            pieces.append(
                (
                    pltpu.make_async_copy(src[k].at[at], held[k].at[at], sems.at[0, k, half]),
                    pltpu.make_async_copy(held[k].at[at], dst[k].at[at], sems.at[1, k, half]),
                )
            )
    for load, _ in pieces:
        load.start()
    for load, store in pieces:
        load.wait()
        store.start()
    for _, store in pieces:
        store.wait()


def per_device(tokens, out_grad, z_weight, router_weight, expert_ids, gate_up_weight, down_weight):
    hbm = pl.BlockSpec(memory_space=pl.ANY)
    dma = pltpu.SemaphoreType.DMA
    outs = pl.pallas_call(
        kernel,
        out_shape=(
            jax.ShapeDtypeStruct((TOK, D), BF),
            jax.ShapeDtypeStruct((SRC, 4, 4, 16, ROUTED), F32),
            jax.ShapeDtypeStruct((D // 16, 2 * FF), BF),
            jax.ShapeDtypeStruct((FF // 16, D), BF),
        ),
        in_specs=[hbm] * 7,
        out_specs=(hbm, hbm, hbm, hbm),
        scratch_shapes=[
            pltpu.VMEM((1, TOK), F32),
            pltpu.VMEM((D, ROUTED), BF),
            pltpu.VMEM((4, TOK), jnp.int32),
            pltpu.VMEM((TOK, D), BF),
            pltpu.VMEM((SRC, 4, 4, 16, ROUTED), F32),
            pltpu.VMEM((D // 16, 2 * FF), BF),
            pltpu.VMEM((FF // 16, D), BF),
            pltpu.VMEM((SRC, TOK, D), BF),
            pltpu.VMEM((SRC, TOK, D), BF),
            pltpu.VMEM((SRC, 16, TOK), F32),
            pltpu.VMEM((TOK, ROUTED), F32),
            pltpu.VMEM((TOK, ROUTED), F32),
            pltpu.VMEM((ROWS, D), BF),
            pltpu.VMEM((D, ROWS), BF),
            pltpu.VMEM((ROWS, D), BF),
            pltpu.VMEM((ROWS, FF), BF),
            pltpu.VMEM((FF, ROWS), BF),
            pltpu.VMEM((ROWS, 2 * FF), BF),
            pltpu.VMEM((D, 2 * FF), BF),
            pltpu.VMEM((FF, D), BF),
            pltpu.VMEM((RING, 2, 16, 128, 128), BF),
            pltpu.VMEM((DEP, 2, 6, 2, 128, 128), BF),
            pltpu.VMEM((DEP, 2, 6, 64, 128), BF),
            pltpu.VMEM((ROWS, D), BF),
            pltpu.VMEM((ROWS, D), BF),
            pltpu.VMEM((ROWS, TOK), BF),
            pltpu.VMEM((ROWS, 1), F32),
            pltpu.VMEM((SRC, 8, TOK), F32),
            pltpu.VMEM((SRC, 8, TOK), F32),
            pltpu.VMEM((TOK, ROUTED), BF),
            pltpu.VMEM((SRC, D // SRC, ROUTED), BF),
            pltpu.VMEM((SRC, D // SRC, ROUTED), BF),
            pltpu.VMEM((4, 4, 16, ROUTED), BF),
            pltpu.VMEM((4, 4, 16, ROUTED), BF),
            pltpu.VMEM((4, 16, ROUTED), BF),
            pltpu.VMEM((4, 16, ROUTED), BF),
            dma((7,)), dma((NG + 3,)),
            dma((6, 14)), dma((6, SRC, 2)),
            dma((SRC,)), dma((SRC,)),
            dma((SRC,)), dma((SRC,)),
            dma((2, SRC)), dma((2, SRC)),
            dma((DEP, 2, 6)), dma((DEP, 2, 6)),
            dma((DEP, 2, 6)), dma((DEP, 2, 6)),
            dma((SRC,)), dma((SRC,)),
            dma((4, 4)), dma((4, 4)),
            dma((SRC, SRC)), dma((SRC,)),
        ],
        compiler_params=pltpu.CompilerParams(
            collective_id=0, has_side_effects=True, vmem_limit_bytes=67043328
        ),
        name="moe_backward",
    )(
        tokens, out_grad, z_weight.reshape(1, TOK), router_weight, expert_ids.T,
        gate_up_weight[0], down_weight[0],
    )
    shapes = tuple(jax.ShapeDtypeStruct(o.shape, o.dtype) for o in outs)
    token_grad, router_grad, gate_up_grad, down_grad = pl.pallas_call(
        write_out,
        out_shape=shapes,
        in_specs=[hbm] * 4,
        out_specs=[hbm] * 4,
        scratch_shapes=[pltpu.VMEM(o.shape, o.dtype) for o in shapes] + [dma((2, 4, 2))],
        name="write_out",
    )(*outs)
    return token_grad, router_grad.reshape(D, ROUTED), gate_up_grad[None], down_grad[None]


def solution(mesh):
    return jax.shard_map(
        per_device,
        mesh=mesh,
        in_specs=(
            P(("dp", "expert"), None),
            P(("dp", "expert"), None),
            P(("dp", "expert")),
            P(),
            P(("dp", "expert"), None),
            P("expert", None, None),
            P("expert", None, None),
        ),
        out_specs=(
            P(("dp", "expert"), None),
            P(),
            P("expert", "dp", None),
            P("expert", "dp", None),
        ),
        check_vma=False,
    )
```
